32 devices in a mesh: parts: 2 (over x), rows: 16 (over z, y, core).
Axes of the slice: x: 2, y: 2, z: 4, core: 2. Of those that a mesh axis runs over, the one named last changes fastest.
Arguments:
- feature_bin: int32 [16384, 700], P(('parts', 'rows')), parts along dimension 0, may hold values from 0 to 255
- doc_leaf: int32 [16384], P(('parts', 'rows')), parts along dimension 0, may hold values from 0 to 31
- current_score: float32 [16384], P(('parts', 'rows')), parts along dimension 0, may hold values from -8 to 8
- relevance: int32 [16384], P(('parts', 'rows')), parts along dimension 0, may hold values from 0 to 4
- doc_rank: int32 [16384], P(('parts', 'rows')), parts along dimension 0, may hold values from 0 to 255, as said below
- query_length: int32 [64], P(('parts', 'rows')), parts along dimension 0, may hold values from 10 to 256, as said below
- feature_votes: int32 [32, 32, 20], P(('parts', 'rows')), parts along dimension 0, may hold values from 0 to 699, all different within a row
- elected: int32 [64, 40], P('parts'), parts along dimension 0, may hold values from 0 to 699, all different within a row
Outputs:
- gradient: float32 [16384], P(('parts', 'rows')), parts along dimension 0
- hessian: float32 [16384], P(('parts', 'rows')), parts along dimension 0
- vote_count: int32 [64, 700], P('parts'), parts along dimension 0
- split_gain: float32 [64, 40, 256], P('parts'), parts along dimension 0
The draws below stay inside these ranges and needn't reach their ends.
There are 2 independent parts, one for each index of `parts`. The reference program is written for one: setup_inputs(seed, part) draws one part's arguments, and reference() takes and returns one part's arrays. A program takes and returns all parts, laid end to end along the dimension named above; each array names one. Nothing has to cross between parts.
Inputs may be any that keep to these rules, and one draw needn't show every extreme that they name: `query_length`: query q holds slots q * 256 to (q + 1) * 256 - 1 of the document arrays; in every draw some query has exactly 256 documents. `doc_rank`: within each query the live documents hold positions 0 to query_length - 1, each once; slots that are not live hold positions from query_length to 255. `feature_votes`: the 20 votes of one device for one leaf are different features. The 40 elected features of one leaf are different.
All inputs are finite; a program needn't handle non-finite values.
Results may differ from the reference program's by a relative error of at most 0.0003.
Values sent between devices are 32-bit elements; how exact they have to be, the bound alone decides.
No kernel may reach another device: no remote copies, remote signals or barrier semaphores. Data moves between devices by JAX's collectives and lax.ppermute only.
A program may use at most 64 MiB of HBM per device.

```python
import jax
import jax.numpy as jnp
from jax import lax

F = 700
B = 256
K = 20
E = 40
LEAVES = 32
QMAX = 256
QDEV = 2
NQ = 32
DOCS = 8192
N_ROWS = 16


def shared_lengths(key):
    base = jax.random.fold_in(key, 11)
    first, second, third = jax.random.split(base, 3)
    devices = NQ // QDEV
    limits = jax.random.randint(first, (devices, 1), QMAX // 4, QMAX - 9)
    extras = jax.random.randint(second, (devices, QDEV), 0, QMAX - 9)
    lengths = (10 + extras % (limits + 1)).reshape(-1)
    longest = jax.random.randint(third, (), 0, NQ)
    lengths = jnp.where(jnp.arange(NQ, dtype=jnp.int32) == longest, QMAX, lengths)
    return lengths.astype(jnp.int32)


def draw_query_length(key, part):
    return shared_lengths(key)


def draw_doc_rank(key, part):
    lengths = shared_lengths(key)
    keys = jax.random.split(jax.random.fold_in(key, 23), NQ)
    orders = jax.vmap(lambda single: jax.random.permutation(single, QMAX))(keys).astype(jnp.int32)
    living = jnp.arange(QMAX, dtype=jnp.int32)[None, :] < lengths[:, None]
    sorting = jnp.where(living, orders, orders + QMAX)
    places = jnp.argsort(jnp.argsort(sorting, axis=1), axis=1)
    return places.reshape(-1).astype(jnp.int32)


def place_ends(drawn, stream_key, least, top_value):
    place = [jax.random.randint(jax.random.fold_in(stream_key, axis), (), 0, length) for axis, length in enumerate(drawn.shape)]
    main_axis = drawn.shape.index(max(drawn.shape))
    neighbour = place[:main_axis] + [(place[main_axis] + 1) % drawn.shape[main_axis]] + place[main_axis + 1:]
    return drawn.at[tuple(place)].set(least).at[tuple(neighbour)].set(top_value)


def level_of(stream_key, extent, pieces, low, high):
    gain = 1.0
    for position, blocks in pieces:
        heights = jax.random.uniform(jax.random.fold_in(jax.random.fold_in(stream_key, 6), position), (blocks,), jnp.float32, low / len(pieces), high / len(pieces))
        gain = gain * jnp.repeat(jnp.exp(heights), extent[position] // blocks).reshape((-1,) + (1,) * (len(extent) - 1 - position))
    return gain


def different_ones(key, rows, count, top, lift):
    order = jax.random.permutation(jax.random.fold_in(key, 1), count)
    pull = order
    for power in range(3):
        pull = pull * pull // count
    pull = pull * lift // count
    lots = jax.random.randint(jax.random.fold_in(key, 2), (rows, count), 0, 4096) + pull
    holders = jax.random.permutation(jax.random.fold_in(key, 3), rows)[jnp.arange(count) % rows]
    lots = jnp.where(jnp.arange(rows)[:, None] == holders[None, :], 1 << 14, lots)
    merit = lots * count + jnp.arange(count)
    return lax.top_k(merit.astype(jnp.int32), top)[1].astype(jnp.int32)


def noise(own_key, dims, width, limit, pieces=(), kind=jnp.bfloat16):
    entries = jax.random.normal(own_key, dims, jnp.float32) * width
    if len(pieces) > 0:
        entries = level_of(own_key, dims, pieces, -0.22, 0.18) * entries
    return jnp.clip(entries, min=-limit, max=limit).astype(kind)


def setup_inputs(seed: int = 0, part: int = 0) -> dict:
    splits = jax.random.split(jax.random.key(seed), 9)
    part_splits = jax.random.split(jax.random.fold_in(splits[8], part), 9)
    feature_bin = place_ends(jax.random.randint(part_splits[0], (DOCS, F), 0, B), jax.random.fold_in(part_splits[0], 1), 0, B - 1).astype(jnp.int32)
    doc_leaf = place_ends(jax.random.randint(part_splits[1], (DOCS,), 0, LEAVES), jax.random.fold_in(part_splits[1], 1), 0, LEAVES - 1).astype(jnp.int32)
    current_score = noise(part_splits[2], (DOCS,), 2.0, 8.0, ((0, 16),), jnp.float32)
    relevance = place_ends(jax.random.randint(part_splits[3], (DOCS,), 0, 5), jax.random.fold_in(part_splits[3], 1), 0, 4).astype(jnp.int32)
    doc_rank = draw_doc_rank(jax.random.fold_in(jax.random.fold_in(splits[8], part), 71), part)
    query_length = draw_query_length(jax.random.fold_in(jax.random.fold_in(splits[8], part), 71), part)
    feature_votes = different_ones(part_splits[6], N_ROWS * LEAVES, F, K, 468).reshape((N_ROWS, LEAVES, K))
    elected = different_ones(part_splits[7], LEAVES, F, E, 0)
    return {"feature_bin": feature_bin, "doc_leaf": doc_leaf, "current_score": current_score, "relevance": relevance, "doc_rank": doc_rank, "query_length": query_length, "feature_votes": feature_votes, "elected": elected}


ridge_weight = 1.0


def query_terms(scores, levels, places, length):
    positions = jnp.arange(scores.shape[0], dtype=jnp.int32)
    living = positions < length
    gains = jnp.exp2(levels.astype(jnp.float32)) - 1.0
    discount = 1.0 / jnp.log2(places.astype(jnp.float32) + 2.0)
    higher = (levels[None, :] > levels[:, None]) & living[None, :]
    earlier = (levels[None, :] == levels[:, None]) & (positions[None, :] < positions[:, None]) & living[None, :]
    ideal_place = jnp.sum((higher | earlier).astype(jnp.float32), axis=1)
    ideal = jnp.sum(jnp.where(living, gains / jnp.log2(ideal_place + 2.0), 0.0))
    scaling = 1.0 / jnp.maximum(ideal, 1.0)
    ordered = (levels[:, None] > levels[None, :]) & living[:, None] & living[None, :]
    chance = jax.nn.sigmoid(scores[None, :] - scores[:, None])
    change = (gains[:, None] - gains[None, :]) * jnp.abs(discount[:, None] - discount[None, :]) * scaling
    pushes = jnp.where(ordered, chance * change, 0.0)
    curves = jnp.where(ordered, chance * (1.0 - chance) * change, 0.0)
    return jnp.sum(pushes, axis=0) - jnp.sum(pushes, axis=1), jnp.sum(curves, axis=0) + jnp.sum(curves, axis=1)


def build_histogram(feature_bin, doc_leaf, gradient, hessian, elected, bins):
    leaves, picked = elected.shape
    columns = elected[doc_leaf]
    chosen = jnp.take_along_axis(feature_bin, columns, axis=1)
    target = (doc_leaf[:, None] * picked + jnp.arange(picked, dtype=jnp.int32)[None, :]) * bins + chosen
    target = target.astype(jnp.int32).reshape(-1)
    segments = leaves * picked * bins
    grad_terms = jnp.broadcast_to(gradient[:, None], (gradient.shape[0], picked)).reshape(-1)
    hess_terms = jnp.broadcast_to(hessian[:, None], (hessian.shape[0], picked)).reshape(-1)
    grad_hist = jax.ops.segment_sum(grad_terms, target, segments)
    hess_hist = jax.ops.segment_sum(hess_terms, target, segments)
    return jnp.stack([grad_hist, hess_hist]).reshape(2, leaves, picked, bins)


def split_score(prefix, whole):
    remain = whole - prefix
    return (prefix[0] * prefix[0] / (prefix[1] + ridge_weight)
            + remain[0] * remain[0] / (remain[1] + ridge_weight)
            - whole[0] * whole[0] / (whole[1] + ridge_weight))


def count_votes(feature_votes, features):
    hits = feature_votes[..., None] == jnp.arange(features, dtype=jnp.int32)
    return jnp.sum(hits.astype(jnp.int32), axis=(0, 2)).astype(jnp.int32)


def reference(feature_bin, doc_leaf, current_score, relevance, doc_rank, query_length, feature_votes, elected):
    def one_query(items):
        return query_terms(items[0], items[1], items[2], items[3])

    gradient, hessian = lax.map(one_query, (current_score.reshape(-1, QMAX), relevance.reshape(-1, QMAX),
                                            doc_rank.reshape(-1, QMAX), query_length))
    gradient = gradient.reshape(-1)
    hessian = hessian.reshape(-1)
    vote_count = count_votes(feature_votes, F)
    histogram = build_histogram(feature_bin, doc_leaf, gradient, hessian, elected, B)
    prefix = jnp.cumsum(histogram, axis=3)
    whole = jnp.sum(histogram, axis=3, keepdims=True)
    split_gain = split_score(prefix, whole)
    return gradient, hessian, vote_count, split_gain
```

```python
import jax
import jax.numpy as jnp
from jax import lax
from jax.experimental import pallas as pl
from jax.experimental.pallas import tpu as pltpu
from jax.sharding import PartitionSpec as P

B = 256
LANES = 128
HALVES = B // LANES
LEVELS = 4

ridge_weight = 1.0


def cdiv(a, b):
    return -(-a // b)


def round_up(a, b):
    return cdiv(a, b) * b


def query_rows(score, level, rank, lengths, slots):
    documents = score.shape[1]
    queries = documents // slots
    gain = jnp.left_shift(1, level).astype(jnp.float32) - 1.0
    discount = 1.0 / jnp.log2(rank.astype(jnp.float32) + 2.0)
    place = lax.broadcasted_iota(jnp.int32, (1, slots), 1)
    place_discount = 1.0 / jnp.log2(place.astype(jnp.float32) + 2.0)
    gradients = []
    hessians = []
    for q in range(queries):
        lanes = slice(q * slots, (q + 1) * slots)
        live = place < lengths[q]
        live_row = live.astype(jnp.float32)
        score_row = score[:, lanes]
        gain_row = gain[:, lanes]
        discount_row = discount[:, lanes]
        level_row = jnp.where(live, level[:, lanes], -1)
        ideal_gain = jnp.zeros((1, slots), jnp.float32)
        for v in range(1, LEVELS + 1):
            count = jnp.sum((level_row >= v).astype(jnp.float32), axis=1, keepdims=True)
            ideal_gain = ideal_gain + jnp.where(
                place.astype(jnp.float32) < count, float(2 ** (v - 1)), 0.0
            )
        ideal = jnp.sum(ideal_gain * place_discount, axis=1, keepdims=True)
        scaling = 1.0 / jnp.maximum(ideal, 1.0)
        rows = jnp.concatenate(
            [score_row, gain_row, discount_row, live_row, jnp.zeros((4, slots), jnp.float32)],
            axis=0,
        )
        columns = rows.T
        step = 32
        push_sum = jnp.zeros((8, slots), jnp.float32)
        curve_sum = jnp.zeros((8, slots), jnp.float32)
        for r in range(0, slots, step):
            part = columns[r : r + step]
            gap = (part[:, 1:2] - gain_row) * part[:, 3:4]
            change = gap * jnp.abs(part[:, 2:3] - discount_row)
            lead = score_row - part[:, 0:1]
            chance = 1.0 / (1.0 + jnp.exp(jnp.where(gap > 0.0, -lead, lead)))
            push = chance * change
            curve = (1.0 - chance) * jnp.abs(push)
            for k in range(0, step, 8):
                push_sum = push_sum + push[k : k + 8]
                curve_sum = curve_sum + curve[k : k + 8]
        factor = scaling * live_row
        gradients.append(jnp.sum(push_sum, axis=0, keepdims=True) * factor)
        hessians.append(jnp.sum(curve_sum, axis=0, keepdims=True) * factor)
    return jnp.concatenate(gradients, axis=1), jnp.concatenate(hessians, axis=1)


def local_stage(bins, leaf, score, level, rank, lengths, votes, elected, plan):
    features, documents = bins.shape
    leaves, picked = elected.shape
    kept = votes.shape[1]
    padded = round_up(picked, 8)
    slots = documents // lengths.shape[0]
    group = 8 if leaves % 8 == 0 else leaves
    per_row = LANES // leaves

    def body(bins_ref, leaf_ref, score_ref, level_ref, rank_ref, length_ref, votes_ref,
             elected_ref, grad_ref, hess_ref, packet_ref, square, chosen_ref):
        square[...] = jnp.zeros(square.shape, jnp.float32)
        square[0:leaves, 0:picked] = elected_ref[...].astype(jnp.float32)
        elected_t = square[...].T
        square[...] = jnp.zeros(square.shape, jnp.float32)
        square[0:leaves, 0:kept] = votes_ref[...].astype(jnp.float32)
        votes_t = square[...].T
        table = bins_ref[...].astype(jnp.float32).astype(jnp.bfloat16)
        leaf_row = leaf_ref[...]
        feature = lax.broadcasted_iota(jnp.int32, (padded, features), 1).astype(jnp.float32)
        chosen = jnp.zeros((padded, documents), jnp.float32)
        for first in range(0, leaves, group):
            picks = []
            for l in range(first, first + group):
                picks.append((elected_t[0:padded, l : l + 1] == feature).astype(jnp.float32))
            hot = jnp.concatenate(picks, axis=0).astype(jnp.bfloat16)
            found = jnp.dot(hot, table, preferred_element_type=jnp.float32)
            for i in range(group):
                chosen = jnp.where(
                    leaf_row == first + i, found[i * padded : (i + 1) * padded], chosen
                )
        chosen_ref[...] = chosen
        gradient, hessian = query_rows(
            score_ref[...], level_ref[...], rank_ref[...], length_ref, slots
        )
        grad_ref[...] = gradient
        hess_ref[...] = hessian
        vote_parts = []
        for k0 in range(0, kept, per_row):
            part = votes_t[k0 : k0 + 1]
            for i in range(1, min(per_row, kept - k0)):
                part = part + pltpu.roll(votes_t[k0 + i : k0 + i + 1], i * leaves, 1)
            vote_parts.append(part)
        while len(vote_parts) * LANES % documents:
            vote_parts.append(jnp.zeros((1, LANES), jnp.float32))
        per = documents // LANES
        shared = [leaf_row.astype(jnp.float32), gradient, hessian]
        for r in range(plan["vote_rows"]):
            shared.append(jnp.concatenate(vote_parts[r * per : (r + 1) * per], axis=1))
        spare = plan["rows"] - plan["picks"] - len(shared)
        if spare:
            shared.append(jnp.zeros((spare, documents), jnp.float32))
        shared = jnp.concatenate(shared, axis=0)
        for j in range(plan["devices"]):
            start = min(j * plan["units"] // HALVES, padded - plan["picks"])
            packet_ref[j, 0 : plan["picks"], :] = chosen_ref[start : start + plan["picks"], :]
            packet_ref[j, plan["picks"] :, :] = shared

    vmem = pl.BlockSpec(memory_space=pltpu.VMEM)
    return pl.pallas_call(
        body,
        in_specs=[vmem] * 5 + [pl.BlockSpec(memory_space=pltpu.SMEM)] + [vmem] * 2,
        out_specs=[vmem] * 3,
        out_shape=[
            jax.ShapeDtypeStruct((1, documents), jnp.float32),
            jax.ShapeDtypeStruct((1, documents), jnp.float32),
            jax.ShapeDtypeStruct((plan["devices"], plan["rows"], documents), jnp.float32),
        ],
        scratch_shapes=[
            pltpu.VMEM((LANES, LANES), jnp.float32),
            pltpu.VMEM((padded, documents), jnp.float32),
        ],
        name="local_stage",
    )(bins, leaf, score, level, rank, lengths, votes, elected)


def gain_stage(packets, where, leaves, plan):
    devices, rows, documents = packets.shape
    picks = plan["picks"]
    units = plan["units"]
    chunk = 4 if devices % 4 == 0 else 1

    def body(where_ref, packet_ref, out_ref):
        base = where_ref[0] * units
        first_pick = base // HALVES
        first_pick = jnp.minimum(first_pick, plan["padded"] - picks)
        leaf_id = lax.broadcasted_iota(jnp.int32, (leaves, documents), 0).astype(jnp.float32)
        bin_id = lax.broadcasted_iota(jnp.int32, (LANES, documents), 0).astype(jnp.float32)
        local = []
        shift = []
        for i in range(units):
            local.append(jnp.clip((base + i) // HALVES - first_pick, 0, picks - 1))
            shift.append((((base + i) % HALVES) * LANES).astype(jnp.float32))
        total = jnp.zeros((4 * leaves, units * LANES), jnp.float32)
        grad_all = jnp.zeros((leaves, documents), jnp.float32)
        hess_all = jnp.zeros((leaves, documents), jnp.float32)
        for s0 in range(0, devices, chunk):
            weights = []
            steps = [[] for _ in range(units)]
            for s in range(s0, s0 + chunk):
                mine = packet_ref[s, picks : picks + 1, :] == leaf_id
                grad = jnp.where(mine, packet_ref[s, picks + 1 : picks + 2, :], 0.0)
                hess = jnp.where(mine, packet_ref[s, picks + 2 : picks + 3, :], 0.0)
                grad_all = grad_all + grad
                hess_all = hess_all + hess
                grad_high = grad.astype(jnp.bfloat16)
                hess_high = hess.astype(jnp.bfloat16)
                grad_low = (grad - grad_high.astype(jnp.float32)).astype(jnp.bfloat16)
                hess_low = (hess - hess_high.astype(jnp.float32)).astype(jnp.bfloat16)
                weights.append(
                    jnp.concatenate([grad_high, hess_high, grad_low, hess_low], axis=0)
                )
                for i in range(units):
                    value = packet_ref[s, pl.ds(local[i], 1), :] - shift[i]
                    steps[i].append((value <= bin_id).astype(jnp.float32).astype(jnp.bfloat16))
            weight = jnp.concatenate(weights, axis=1)
            step = jnp.concatenate([jnp.concatenate(p, axis=1) for p in steps], axis=0)
            total = total + lax.dot_general(
                weight, step, (((1,), (1,)), ((), ())), preferred_element_type=jnp.float32
            )
        prefix_grad = total[0:leaves] + total[2 * leaves : 3 * leaves]
        prefix_hess = total[leaves : 2 * leaves] + total[3 * leaves :]
        whole_grad = jnp.sum(grad_all, axis=1, keepdims=True)
        whole_hess = jnp.sum(hess_all, axis=1, keepdims=True)
        rest_grad = whole_grad - prefix_grad
        rest_hess = whole_hess - prefix_hess
        gains = (
            prefix_grad * prefix_grad / (prefix_hess + ridge_weight)
            + rest_grad * rest_grad / (rest_hess + ridge_weight)
            - whole_grad * whole_grad / (whole_hess + ridge_weight)
        )
        for i in range(units):
            out_ref[i * leaves : (i + 1) * leaves, :] = gains[:, i * LANES : (i + 1) * LANES]

    vmem = pl.BlockSpec(memory_space=pltpu.VMEM)
    return pl.pallas_call(
        body,
        in_specs=[pl.BlockSpec(memory_space=pltpu.SMEM), vmem],
        out_specs=vmem,
        out_shape=jax.ShapeDtypeStruct((units * leaves, LANES), jnp.float32),
        name="gain_stage",
    )(where, packets)


def vote_stage(packets, features, leaves, kept, plan):
    devices, rows, documents = packets.shape
    first_row = plan["picks"] + 3
    lines = cdiv(kept * leaves, LANES)
    per = documents // LANES
    padded = round_up(features, 8)
    step = 64

    def body(packet_ref, out_ref, count):
        lane = lax.broadcasted_iota(jnp.int32, (1, LANES), 1)

        def block(index, carry):
            start = pl.multiple_of(index * step, step)
            feature = (lax.broadcasted_iota(jnp.int32, (step, LANES), 0) + start).astype(
                jnp.float32
            )
            total = jnp.zeros((step, LANES), jnp.float32)
            for s in range(devices):
                for line in range(lines):
                    row = first_row + line // per
                    col = (line % per) * LANES
                    values = packet_ref[s, row : row + 1, col : col + LANES]
                    inside = kept * leaves - line * LANES
                    if inside < LANES:
                        values = jnp.where(lane < inside, values, -1.0)
                    total = total + (values == feature).astype(jnp.float32)
            count[pl.ds(start, step), :] = total
            return carry

        lax.fori_loop(0, cdiv(padded, step), block, 0)
        turned = count[...].T
        summed = turned[0:leaves]
        for i in range(1, LANES // leaves):
            summed = summed + turned[i * leaves : (i + 1) * leaves]
        out_ref[...] = summed[:, 0:features].astype(jnp.int32)

    vmem = pl.BlockSpec(memory_space=pltpu.VMEM)
    depth = round_up(round_up(padded, step), LANES)
    return pl.pallas_call(
        body,
        in_specs=[vmem],
        out_specs=vmem,
        out_shape=jax.ShapeDtypeStruct((leaves, features), jnp.int32),
        scratch_shapes=[pltpu.VMEM((depth, LANES), jnp.float32)],
        name="vote_stage",
    )(packets)


def place_stage(blocks, where, leaves, picked, plan):
    units = plan["units"]

    def body(where_ref, block_ref, out_ref):
        here = where_ref[0]
        for unit in range(picked * HALVES):
            slot = unit // units
            if plan["bits"]:
                offset = here ^ slot
                slot = 0
                for position, bit in enumerate(plan["bits"]):
                    slot = slot + jnp.where((offset & bit) != 0, 1 << position, 0)
            start = pl.multiple_of((slot * units + unit % units) * leaves, leaves)
            lane = (unit % HALVES) * LANES
            out_ref[:, unit // HALVES, lane : lane + LANES] = block_ref[pl.ds(start, leaves), :]

    vmem = pl.BlockSpec(memory_space=pltpu.VMEM)
    return pl.pallas_call(
        body,
        in_specs=[pl.BlockSpec(memory_space=pltpu.SMEM), vmem],
        out_specs=vmem,
        out_shape=jax.ShapeDtypeStruct((leaves, picked, B), jnp.float32),
        name="place_stage",
    )(where, blocks)


def solution(mesh):
    devices = mesh.shape["rows"]

    def on_device(
        feature_bin, doc_leaf, current_score, relevance, doc_rank, query_length, feature_votes,
        elected,
    ):
        documents, features = feature_bin.shape
        leaves, picked = elected.shape
        kept = feature_votes.shape[2]
        units = cdiv(picked * HALVES, devices)
        padded = round_up(picked, 8)
        picks = max(
            (j * units + units - 1) // HALVES - (j * units) // HALVES + 1 for j in range(devices)
        )
        vote_rows = cdiv(kept * leaves, documents)
        plan = {
            "devices": devices,
            "units": units,
            "picks": picks,
            "padded": padded,
            "vote_rows": vote_rows,
            "rows": round_up(picks + 3 + vote_rows, 8),
            "bits": None,
        }
        where = lax.axis_index("rows").astype(jnp.int32).reshape(1)
        gradient, hessian, packets = local_stage(
            feature_bin.T,
            doc_leaf.reshape(1, -1),
            current_score.reshape(1, -1),
            relevance.reshape(1, -1),
            doc_rank.reshape(1, -1),
            query_length,
            feature_votes.reshape(leaves, kept),
            elected,
            plan,
        )
        received = lax.all_to_all(packets, "rows", 0, 0)
        block = gain_stage(received, where, leaves, plan)
        vote_count = vote_stage(received, features, leaves, kept, plan)
        if devices & (devices - 1) == 0 and devices > 1:
            gathered = block
            plan["bits"] = [1 << b for b in reversed(range(devices.bit_length() - 1))]
            for bit in plan["bits"]:
                other = lax.ppermute(gathered, "rows", [(i, i ^ bit) for i in range(devices)])
                gathered = jnp.concatenate([gathered, other], axis=0)
        else:
            gathered = lax.all_gather(block, "rows", axis=0, tiled=True)
        split_gain = place_stage(gathered, where, leaves, picked, plan)
        return gradient.reshape(-1), hessian.reshape(-1), vote_count, split_gain

    return jax.shard_map(
        on_device,
        mesh=mesh,
        in_specs=(
            P(("parts", "rows"), None),
            P(("parts", "rows")),
            P(("parts", "rows")),
            P(("parts", "rows")),
            P(("parts", "rows")),
            P(("parts", "rows")),
            P(("parts", "rows"), None, None),
            P("parts", None),
        ),
        out_specs=(
            P(("parts", "rows")),
            P(("parts", "rows")),
            P("parts", None),
            P("parts", None, None),
        ),
        check_vma=False,
    )
```

```python
import jax
import jax.numpy as jnp
from jax import lax
from jax.experimental import pallas as pl
from jax.experimental.pallas import tpu as pltpu
from jax.sharding import PartitionSpec as P

B = 256
LANES = 128
HALVES = B // LANES
LEVELS = 4

ridge_weight = 1.0


def cdiv(a, b):
    return -(-a // b)


def round_up(a, b):
    return cdiv(a, b) * b


def query_rows(score, level, rank, lengths, slots):
    documents = score.shape[1]
    queries = documents // slots
    gain = jnp.left_shift(1, level).astype(jnp.float32) - 1.0
    discount = 1.0 / jnp.log2(rank.astype(jnp.float32) + 2.0)
    place = lax.broadcasted_iota(jnp.int32, (1, slots), 1)
    place_discount = 1.0 / jnp.log2(place.astype(jnp.float32) + 2.0)
    gradients = []
    hessians = []
    for q in range(queries):
        lanes = slice(q * slots, (q + 1) * slots)
        live = place < lengths[q]
        live_row = live.astype(jnp.float32)
        score_row = score[:, lanes]
        gain_row = gain[:, lanes]
        discount_row = discount[:, lanes]
        level_row = jnp.where(live, level[:, lanes], -1)
        ideal_gain = jnp.zeros((1, slots), jnp.float32)
        for v in range(1, LEVELS + 1):
            count = jnp.sum((level_row >= v).astype(jnp.float32), axis=1, keepdims=True)
            ideal_gain = ideal_gain + jnp.where(
                place.astype(jnp.float32) < count, float(2 ** (v - 1)), 0.0
            )
        ideal = jnp.sum(ideal_gain * place_discount, axis=1, keepdims=True)
        scaling = 1.0 / jnp.maximum(ideal, 1.0)
        rows = jnp.concatenate(
            [score_row, gain_row, discount_row, live_row, jnp.zeros((4, slots), jnp.float32)],
            axis=0,
        )
        columns = rows.T
        step = 32
        push_sum = jnp.zeros((8, slots), jnp.float32)
        curve_sum = jnp.zeros((8, slots), jnp.float32)
        for r in range(0, slots, step):
            part = columns[r : r + step]
            gap = (part[:, 1:2] - gain_row) * part[:, 3:4]
            change = gap * jnp.abs(part[:, 2:3] - discount_row)
            lead = score_row - part[:, 0:1]
            chance = 1.0 / (1.0 + jnp.exp(jnp.where(gap > 0.0, -lead, lead)))
            push = chance * change
            curve = (1.0 - chance) * jnp.abs(push)
            for k in range(0, step, 8):
                push_sum = push_sum + push[k : k + 8]
                curve_sum = curve_sum + curve[k : k + 8]
        factor = scaling * live_row
        gradients.append(jnp.sum(push_sum, axis=0, keepdims=True) * factor)
        hessians.append(jnp.sum(curve_sum, axis=0, keepdims=True) * factor)
    return jnp.concatenate(gradients, axis=1), jnp.concatenate(hessians, axis=1)


def vmem_array(shape):
    return pltpu.VMEM(shape, jnp.float32)


def in_vmem(x):
    return pltpu.with_memory_space_constraint(x, pltpu.VMEM)


def in_hbm(x):
    return pltpu.with_memory_space_constraint(x, pltpu.HBM)


def local_stage(bins, leaf, score, level, rank, lengths, votes, elected, plan):
    features, documents = bins.shape
    leaves, picked = elected.shape
    kept = votes.shape[0]
    padded = plan["padded"]
    picks = plan["picks"]
    rows = plan["rows"]
    slots = documents // lengths.shape[0]
    group = 8 if leaves % 8 == 0 else leaves
    per_row = LANES // leaves

    def body(bins_ref, leaf_ref, score_ref, level_ref, rank_ref, length_ref, votes_ref,
             elected_ref, grad_ref, hess_ref, packet_ref, square, chosen_ref):
        square[...] = jnp.zeros(square.shape, jnp.float32)
        square[0:leaves, 0:picked] = elected_ref[...].astype(jnp.float32)
        elected_t = square[...].T
        table = bins_ref[...].astype(jnp.float32).astype(jnp.bfloat16)
        leaf_row = leaf_ref[...]
        feature = lax.broadcasted_iota(jnp.int32, (padded, features), 1).astype(jnp.float32)
        chosen = jnp.zeros((padded, documents), jnp.float32)
        for first in range(0, leaves, group):
            hot = []
            for l in range(first, first + group):
                hot.append((elected_t[0:padded, l : l + 1] == feature).astype(jnp.float32))
            hot = jnp.concatenate(hot, axis=0).astype(jnp.bfloat16)
            found = jnp.dot(hot, table, preferred_element_type=jnp.float32)
            for i in range(group):
                chosen = jnp.where(
                    leaf_row == first + i, found[i * padded : (i + 1) * padded], chosen
                )
        chosen_ref[...] = chosen
        gradient, hessian = query_rows(
            score_ref[...], level_ref[...], rank_ref[...], length_ref, slots
        )
        grad_ref[...] = gradient
        hess_ref[...] = hessian
        tail = []
        for k0 in range(0, kept, per_row):
            line = jnp.zeros((1, LANES), jnp.float32)
            for i in range(min(per_row, kept - k0)):
                values = votes_ref[k0 + i].astype(jnp.float32)
                pieces = [values]
                if i:
                    pieces.insert(0, jnp.zeros((1, i * leaves), jnp.float32))
                if (i + 1) * leaves < LANES:
                    pieces.append(jnp.zeros((1, LANES - (i + 1) * leaves), jnp.float32))
                line = line + jnp.concatenate(pieces, axis=1)
            tail.append(line)
        spare = plan["vote_tiles"] * rows - len(tail)
        if spare:
            tail.append(jnp.zeros((spare, LANES), jnp.float32))
        tail = jnp.concatenate(tail, axis=0)
        shared = [leaf_row.astype(jnp.float32), gradient, hessian]
        if rows > picks + 3:
            shared.append(jnp.zeros((rows - picks - 3, documents), jnp.float32))
        shared = jnp.concatenate(shared, axis=0)
        for j in range(plan["devices"]):
            start = plan["first"][j % plan["owners"]]
            block = jnp.concatenate([chosen_ref[start : start + picks, :], shared], axis=0)
            for c in range(documents // LANES):
                packet_ref[j, c] = block[:, c * LANES : (c + 1) * LANES]
            for t in range(plan["vote_tiles"]):
                packet_ref[j, documents // LANES + t] = tail[t * rows : (t + 1) * rows]

    vmem = pl.BlockSpec(memory_space=pltpu.VMEM)
    return pl.pallas_call(
        body,
        in_specs=[vmem] * 5 + [pl.BlockSpec(memory_space=pltpu.SMEM)] + [vmem] * 2,
        out_specs=[vmem] * 3,
        out_shape=[
            jax.ShapeDtypeStruct((1, documents), jnp.float32),
            jax.ShapeDtypeStruct((1, documents), jnp.float32),
            vmem_array(
                (plan["devices"], documents // LANES + plan["vote_tiles"], rows, LANES)
            ),
        ],
        scratch_shapes=[
            pltpu.VMEM((LANES, LANES), jnp.float32),
            pltpu.VMEM((padded, documents), jnp.float32),
        ],
        compiler_params=pltpu.CompilerParams(vmem_limit_bytes=48 << 20),
        name="local_stage",
    )(*[in_hbm(x) for x in (bins, leaf, score, level, rank, lengths, votes, elected)])


def gain_stage(packets, where, leaves, plan):
    devices = packets.shape[0]
    picks = plan["picks"]
    units = plan["units"]
    chunks = plan["chunks"]
    chunk = 4 if devices % 4 == 0 else 1
    even = units % HALVES == 0

    def body(where_ref, packet_ref, out_ref):
        leaf_id = lax.broadcasted_iota(jnp.int32, (leaves, LANES), 0).astype(jnp.float32)
        bin_id = lax.broadcasted_iota(jnp.int32, (LANES, LANES), 0).astype(jnp.float32)
        local = []
        limit = []
        base = where_ref[0] % plan["owners"] * units
        first = jnp.minimum(base // HALVES, plan["padded"] - picks)
        for i in range(units):
            if even:
                local.append(i // HALVES)
                limit.append(bin_id + float(i % HALVES * LANES))
            else:
                local.append(jnp.clip((base + i) // HALVES - first, 0, picks - 1))
                limit.append(bin_id + ((base + i) % HALVES * LANES).astype(jnp.float32))
        total = jnp.zeros((4 * leaves, units * LANES), jnp.float32)
        grad_all = jnp.zeros((leaves, LANES), jnp.float32)
        hess_all = jnp.zeros((leaves, LANES), jnp.float32)
        for s0 in range(0, devices, chunk):
            weights = []
            steps = [[] for _ in range(units)]
            for s in range(s0, s0 + chunk):
                for c in range(chunks):
                    mine = packet_ref[s, c, picks : picks + 1, :] == leaf_id
                    grad = jnp.where(mine, packet_ref[s, c, picks + 1 : picks + 2, :], 0.0)
                    hess = jnp.where(mine, packet_ref[s, c, picks + 2 : picks + 3, :], 0.0)
                    grad_all = grad_all + grad
                    hess_all = hess_all + hess
                    grad_high = grad.astype(jnp.bfloat16)
                    hess_high = hess.astype(jnp.bfloat16)
                    grad_low = (grad - grad_high.astype(jnp.float32)).astype(jnp.bfloat16)
                    hess_low = (hess - hess_high.astype(jnp.float32)).astype(jnp.bfloat16)
                    weights.append(
                        jnp.concatenate([grad_high, hess_high, grad_low, hess_low], axis=0)
                    )
                    for i in range(units):
                        value = packet_ref[s, c, pl.ds(local[i], 1), :]
                        steps[i].append(
                            (value <= limit[i]).astype(jnp.float32).astype(jnp.bfloat16)
                        )
            weight = jnp.concatenate(weights, axis=1)
            step = jnp.concatenate([jnp.concatenate(p, axis=1) for p in steps], axis=0)
            total = total + lax.dot_general(
                weight, step, (((1,), (1,)), ((), ())), preferred_element_type=jnp.float32
            )
        prefix_grad = total[0:leaves] + total[2 * leaves : 3 * leaves]
        prefix_hess = total[leaves : 2 * leaves] + total[3 * leaves :]
        whole_grad = jnp.sum(grad_all, axis=1, keepdims=True)
        whole_hess = jnp.sum(hess_all, axis=1, keepdims=True)
        rest_grad = whole_grad - prefix_grad
        rest_hess = whole_hess - prefix_hess
        gains = (
            prefix_grad * prefix_grad / (prefix_hess + ridge_weight)
            + rest_grad * rest_grad / (rest_hess + ridge_weight)
            - whole_grad * whole_grad / (whole_hess + ridge_weight)
        )
        for i in range(units):
            out_ref[i * leaves : (i + 1) * leaves, :] = gains[:, i * LANES : (i + 1) * LANES]

    vmem = pl.BlockSpec(memory_space=pltpu.VMEM)
    return pl.pallas_call(
        body,
        in_specs=[pl.BlockSpec(memory_space=pltpu.SMEM), vmem],
        out_specs=vmem,
        out_shape=vmem_array((units * leaves, LANES)),
        compiler_params=pltpu.CompilerParams(vmem_limit_bytes=48 << 20),
        name="gain_stage",
    )(where, in_vmem(packets))


def vote_stage(packets, features, leaves, kept, plan):
    devices = packets.shape[0]
    rows = plan["rows"]
    lines = cdiv(kept * leaves, LANES)
    padded = round_up(features, 8)
    step = 64
    depth = round_up(padded, LANES)

    def body(packet_ref, out_ref, count):
        lane = lax.broadcasted_iota(jnp.int32, (1, LANES), 1)

        def block(index, carry):
            start = pl.multiple_of(index * step, step)
            feature = (lax.broadcasted_iota(jnp.int32, (step, LANES), 0) + start).astype(
                jnp.float32
            )
            total = jnp.zeros((step, LANES), jnp.float32)
            for s in range(devices):
                for line in range(lines):
                    row = line % rows
                    values = packet_ref[s, plan["chunks"] + line // rows, row : row + 1, :]
                    inside = kept * leaves - line * LANES
                    if inside < LANES:
                        values = jnp.where(lane < inside, values, -1.0)
                    total = total + (values == feature).astype(jnp.float32)
            count[pl.ds(start, step), :] = total
            return carry

        lax.fori_loop(0, depth // step, block, 0)
        turned = count[...].T
        summed = turned[0:leaves]
        for i in range(1, LANES // leaves):
            summed = summed + turned[i * leaves : (i + 1) * leaves]
        out_ref[...] = summed[:, 0:features].astype(jnp.int32)

    vmem = pl.BlockSpec(memory_space=pltpu.VMEM)
    return pl.pallas_call(
        body,
        in_specs=[vmem],
        out_specs=vmem,
        out_shape=jax.ShapeDtypeStruct((leaves, features), jnp.int32),
        scratch_shapes=[pltpu.VMEM((depth, LANES), jnp.float32)],
        compiler_params=pltpu.CompilerParams(vmem_limit_bytes=48 << 20),
        cost_estimate=pl.CostEstimate(flops=40_000_000, bytes_accessed=400_000, transcendentals=0),
        name="vote_stage",
    )(in_vmem(packets))


def place_stage(blocks, where, leaves, picked, plan):
    units = plan["units"]
    owners = plan["owners"]
    step = 8 if leaves % 8 == 0 else leaves

    def body(where_ref, *refs):
        out_ref = refs[-1]
        here = where_ref[0] % owners
        first = pl.program_id(0) * step
        odd = here & 1
        for index, ref in enumerate(refs[:-1]):
            owner = index
            if plan["doubling"]:
                near, far = plan["tags"][index % len(plan["tags"])]
                if index < len(plan["tags"]):
                    owner = here ^ jnp.where(odd == 1, far, near)
                else:
                    owner = here ^ 1 ^ jnp.where(odd == 1, near, far)

            def write(target, ref=ref):
                for i in range(units):
                    unit = target * units + i
                    if unit < picked * HALVES:
                        start = pl.multiple_of(i * leaves + first, step)
                        lane = unit % HALVES * LANES
                        out_ref[:, unit // HALVES, lane : lane + LANES] = ref[
                            pl.ds(start, step), :
                        ]

            if plan["doubling"]:
                for target in range(owners):
                    pl.when(owner == target)(lambda target=target, write=write: write(target))
            else:
                write(owner)

    vmem = pl.BlockSpec(memory_space=pltpu.VMEM)
    return pl.pallas_call(
        body,
        grid=(leaves // step,),
        in_specs=[pl.BlockSpec(memory_space=pltpu.SMEM)] + [vmem] * len(blocks),
        out_specs=pl.BlockSpec((step, picked, B), lambda i: (i, 0, 0)),
        out_shape=jax.ShapeDtypeStruct((leaves, picked, B), jnp.float32),
        compiler_params=pltpu.CompilerParams(vmem_limit_bytes=48 << 20),
        name="place_stage",
    )(where, *[in_vmem(b) for b in blocks])


def solution(mesh):
    devices = mesh.shape["rows"]

    def on_device(
        feature_bin, doc_leaf, current_score, relevance, doc_rank, query_length, feature_votes,
        elected,
    ):
        documents, features = feature_bin.shape
        leaves, picked = elected.shape
        kept = feature_votes.shape[2]
        doubling = devices >= 8 and devices & (devices - 1) == 0
        owners = devices // 2 if doubling else devices
        units = cdiv(picked * HALVES, owners)
        padded = round_up(picked, 8)
        picks = max(
            (j * units + units - 1) // HALVES - (j * units) // HALVES + 1 for j in range(owners)
        )
        rows = round_up(picks + 3, 8)
        plan = {
            "devices": devices,
            "doubling": doubling,
            "owners": owners,
            "units": units,
            "picks": picks,
            "padded": padded,
            "first": [min(j * units // HALVES, padded - picks) for j in range(owners)],
            "rows": rows,
            "chunks": documents // LANES,
            "vote_tiles": cdiv(cdiv(kept * leaves, LANES), rows),
        }
        where = lax.axis_index("rows").astype(jnp.int32).reshape(1)
        gradient, hessian, packets = local_stage(
            feature_bin.T,
            doc_leaf.reshape(1, -1),
            current_score.reshape(1, -1),
            relevance.reshape(1, -1),
            doc_rank.reshape(1, -1),
            query_length,
            feature_votes.transpose(2, 0, 1),
            elected,
            plan,
        )
        received = lax.all_to_all(packets, "rows", 0, 0)
        block = gain_stage(received, where, leaves, plan)
        vote_count = vote_stage(received, features, leaves, kept, plan)
        if doubling:
            far = [1 << b for b in reversed(range(1, owners.bit_length() - 1))]
            twin = list(far)
            twin[-2:] = twin[-2:][::-1]
            pairs = [
                [(i, i ^ (twin[p] if i & 1 else far[p])) for i in range(devices)]
                for p in range(len(far))
            ]
            blocks = [block]
            tags = [(0, 0)]
            for p in range(len(far)):
                moved = [lax.ppermute(b, "rows", pairs[p]) for b in blocks]
                if p == 0:
                    moved[0], vote_count = lax.optimization_barrier((moved[0], vote_count))
                blocks = blocks + moved
                tags = tags + [(even | far[p], odd | twin[p]) for even, odd in tags]
            sibling = [(i, i ^ 1) for i in range(devices)]
            blocks = blocks + [lax.ppermute(b, "rows", sibling) for b in blocks]
            plan["tags"] = tags
        else:
            gathered = lax.all_gather(block, "rows", axis=0)
            blocks = [gathered[j] for j in range(devices)]
            plan["tags"] = None
        split_gain = place_stage(blocks, where, leaves, picked, plan)
        return gradient.reshape(-1), hessian.reshape(-1), vote_count, split_gain

    return jax.shard_map(
        on_device,
        mesh=mesh,
        in_specs=(
            P(("parts", "rows"), None),
            P(("parts", "rows")),
            P(("parts", "rows")),
            P(("parts", "rows")),
            P(("parts", "rows")),
            P(("parts", "rows")),
            P(("parts", "rows"), None, None),
            P("parts", None),
        ),
        out_specs=(
            P(("parts", "rows")),
            P(("parts", "rows")),
            P("parts", None),
            P("parts", None, None),
        ),
        check_vma=False,
    )
```

```python
import jax
import jax.numpy as jnp
from jax import lax
from jax.experimental import pallas as pl
from jax.experimental.pallas import tpu as pltpu
from jax.sharding import PartitionSpec as P

B = 256
LANES = 128
HALVES = B // LANES
LEVELS = 4

ridge_weight = 1.0


def cdiv(a, b):
    return -(-a // b)


def round_up(a, b):
    return cdiv(a, b) * b


def query_rows(score, level, rank, lengths, slots):
    documents = score.shape[1]
    queries = documents // slots
    gain = jnp.left_shift(1, level).astype(jnp.float32) - 1.0
    discount = 1.0 / jnp.log2(rank.astype(jnp.float32) + 2.0)
    place = lax.broadcasted_iota(jnp.int32, (1, slots), 1)
    place_discount = 1.0 / jnp.log2(place.astype(jnp.float32) + 2.0)
    gradients = []
    hessians = []
    for q in range(queries):
        lanes = slice(q * slots, (q + 1) * slots)
        live = place < lengths[q]
        live_row = live.astype(jnp.float32)
        score_row = score[:, lanes]
        gain_row = gain[:, lanes]
        discount_row = discount[:, lanes]
        level_row = jnp.where(live, level[:, lanes], -1)
        ideal_gain = jnp.zeros((1, slots), jnp.float32)
        for v in range(1, LEVELS + 1):
            count = jnp.sum((level_row >= v).astype(jnp.float32), axis=1, keepdims=True)
            ideal_gain = ideal_gain + jnp.where(
                place.astype(jnp.float32) < count, float(2 ** (v - 1)), 0.0
            )
        ideal = jnp.sum(ideal_gain * place_discount, axis=1, keepdims=True)
        scaling = 1.0 / jnp.maximum(ideal, 1.0)
        rows = jnp.concatenate(
            [score_row, gain_row, discount_row, live_row, jnp.zeros((4, slots), jnp.float32)],
            axis=0,
        )
        columns = rows.T
        step = 32
        push_sum = jnp.zeros((8, slots), jnp.float32)
        curve_sum = jnp.zeros((8, slots), jnp.float32)
        for r in range(0, slots, step):
            part = columns[r : r + step]
            gap = (part[:, 1:2] - gain_row) * part[:, 3:4]
            change = gap * jnp.abs(part[:, 2:3] - discount_row)
            lead = score_row - part[:, 0:1]
            chance = 1.0 / (1.0 + jnp.exp(jnp.where(gap > 0.0, -lead, lead)))
            push = chance * change
            curve = (1.0 - chance) * jnp.abs(push)
            for k in range(0, step, 8):
                push_sum = push_sum + push[k : k + 8]
                curve_sum = curve_sum + curve[k : k + 8]
        factor = scaling * live_row
        gradients.append(jnp.sum(push_sum, axis=0, keepdims=True) * factor)
        hessians.append(jnp.sum(curve_sum, axis=0, keepdims=True) * factor)
    return jnp.concatenate(gradients, axis=1), jnp.concatenate(hessians, axis=1)


def vmem_array(shape):
    return pltpu.VMEM(shape, jnp.float32)


def in_vmem(x):
    return pltpu.with_memory_space_constraint(x, pltpu.VMEM)


def in_hbm(x):
    return pltpu.with_memory_space_constraint(x, pltpu.HBM)


def local_stage(bins, leaf, score, level, rank, lengths, votes, elected, plan):
    features, documents = bins.shape
    leaves, picked = elected.shape
    kept = votes.shape[0]
    padded = plan["padded"]
    picks = plan["picks"]
    rows = plan["rows"]
    slots = documents // lengths.shape[0]
    group = 8 if leaves % 8 == 0 else leaves
    per_row = LANES // leaves

    def body(bins_ref, leaf_ref, score_ref, level_ref, rank_ref, length_ref, votes_ref,
             elected_ref, grad_ref, hess_ref, packet_ref, square, chosen_ref, bins_here, arrived):
        fetch = pltpu.make_async_copy(bins_ref, bins_here, arrived)
        fetch.start()
        square[...] = jnp.zeros(square.shape, jnp.float32)
        square[0:leaves, 0:picked] = elected_ref[...].astype(jnp.float32)
        elected_t = square[...].T
        leaf_row = leaf_ref[...]
        gradient, hessian = query_rows(
            score_ref[...], level_ref[...], rank_ref[...], length_ref, slots
        )
        grad_ref[...] = gradient
        hess_ref[...] = hessian
        lane = lax.broadcasted_iota(jnp.int32, (1, documents), 1)
        starts = [0]
        for q in range(documents // slots):
            starts.append(starts[-1] + length_ref[q])

        def compact(block):
            result = block
            for q in range(1, documents // slots):
                moved = pltpu.roll(block, starts[q] - q * slots + documents, 1)
                result = jnp.where(lane >= starts[q], moved, result)
            return result

        shared = [leaf_row.astype(jnp.float32), gradient, hessian]
        shared.append(jnp.zeros((max(rows - picks, 8) - 3, documents), jnp.float32))
        shared = compact(jnp.concatenate(shared, axis=0))[0 : rows - picks]
        shared = jnp.where(lane < starts[-1], shared, 0.0)
        count = jnp.zeros((1, LANES), jnp.float32) + starts[-1].astype(jnp.float32)
        fetch.wait()
        table = bins_here[...].astype(jnp.float32).astype(jnp.bfloat16)
        feature = lax.broadcasted_iota(jnp.int32, (padded, features), 1).astype(jnp.float32)
        chosen = jnp.zeros((padded, documents), jnp.float32)
        for first in range(0, leaves, group):
            hot = []
            for l in range(first, first + group):
                hot.append((elected_t[0:padded, l : l + 1] == feature).astype(jnp.float32))
            hot = jnp.concatenate(hot, axis=0).astype(jnp.bfloat16)
            found = jnp.dot(hot, table, preferred_element_type=jnp.float32)
            for i in range(group):
                chosen = jnp.where(
                    leaf_row == first + i, found[i * padded : (i + 1) * padded], chosen
                )
        chosen_ref[...] = compact(chosen)
        tail = []
        for k0 in range(0, kept, per_row):
            line = jnp.zeros((1, LANES), jnp.float32)
            for i in range(min(per_row, kept - k0)):
                values = votes_ref[k0 + i].astype(jnp.float32)
                pieces = [values]
                if i:
                    pieces.insert(0, jnp.zeros((1, i * leaves), jnp.float32))
                if (i + 1) * leaves < LANES:
                    pieces.append(jnp.zeros((1, LANES - (i + 1) * leaves), jnp.float32))
                line = line + jnp.concatenate(pieces, axis=1)
            tail.append(line)
        tail.append(count)
        spare = plan["vote_tiles"] * rows - len(tail)
        if spare:
            tail.append(jnp.zeros((spare, LANES), jnp.float32))
        tail = jnp.concatenate(tail, axis=0)
        for j in range(plan["devices"]):
            start = plan["first"][j % plan["owners"]]
            block = jnp.concatenate([chosen_ref[start : start + picks, :], shared], axis=0)
            for c in range(documents // LANES):
                packet_ref[j, c] = block[:, c * LANES : (c + 1) * LANES]
            for t in range(plan["vote_tiles"]):
                packet_ref[j, documents // LANES + t] = tail[t * rows : (t + 1) * rows]

    vmem = pl.BlockSpec(memory_space=pltpu.VMEM)
    return pl.pallas_call(
        body,
        in_specs=[pl.BlockSpec(memory_space=pltpu.HBM)]
        + [vmem] * 4
        + [pl.BlockSpec(memory_space=pltpu.SMEM)]
        + [vmem] * 2,
        out_specs=[vmem] * 3,
        out_shape=[
            jax.ShapeDtypeStruct((1, documents), jnp.float32),
            jax.ShapeDtypeStruct((1, documents), jnp.float32),
            vmem_array(
                (plan["devices"], documents // LANES + plan["vote_tiles"], rows, LANES)
            ),
        ],
        scratch_shapes=[
            pltpu.VMEM((LANES, LANES), jnp.float32),
            pltpu.VMEM((padded, documents), jnp.float32),
            pltpu.VMEM((features, documents), jnp.int32),
            pltpu.SemaphoreType.DMA,
        ],
        compiler_params=pltpu.CompilerParams(vmem_limit_bytes=48 << 20),
        name="local_stage",
    )(*[in_hbm(x) for x in (bins, leaf, score, level, rank, lengths, votes, elected)])


def gain_stage(packets, where, leaves, plan):
    devices = packets.shape[0]
    picks = plan["picks"]
    units = plan["units"]
    chunks = plan["chunks"]
    chunk = 4 if devices % 4 == 0 else 1
    even = units % HALVES == 0

    half = cdiv(chunks, 2)

    def body(where_ref, packet_ref, out_ref, total_ref, grad_ref, hess_ref):
        leaf_id = lax.broadcasted_iota(jnp.int32, (leaves, LANES), 0).astype(jnp.float32)
        bin_id = lax.broadcasted_iota(jnp.int32, (LANES, LANES), 0).astype(jnp.float32)
        local = []
        limit = []
        base = where_ref[0] % plan["owners"] * units
        first = jnp.minimum(base // HALVES, plan["padded"] - picks)
        for i in range(units):
            if even:
                local.append(i // HALVES)
                limit.append(bin_id + float(i % HALVES * LANES))
            else:
                local.append(jnp.clip((base + i) // HALVES - first, 0, picks - 1))
                limit.append(bin_id + ((base + i) % HALVES * LANES).astype(jnp.float32))
        def terms(sources, parts):
            weights = []
            steps = [[] for _ in range(units)]
            grad_sum = jnp.zeros((leaves, LANES), jnp.float32)
            hess_sum = jnp.zeros((leaves, LANES), jnp.float32)
            for s in sources:
                for c in parts:
                    mine = packet_ref[s, c, picks : picks + 1, :] == leaf_id
                    grad = jnp.where(mine, packet_ref[s, c, picks + 1 : picks + 2, :], 0.0)
                    hess = jnp.where(mine, packet_ref[s, c, picks + 2 : picks + 3, :], 0.0)
                    grad_sum = grad_sum + grad
                    hess_sum = hess_sum + hess
                    grad_high = grad.astype(jnp.bfloat16)
                    hess_high = hess.astype(jnp.bfloat16)
                    grad_low = (grad - grad_high.astype(jnp.float32)).astype(jnp.bfloat16)
                    hess_low = (hess - hess_high.astype(jnp.float32)).astype(jnp.bfloat16)
                    weights.append(
                        jnp.concatenate([grad_high, hess_high, grad_low, hess_low], axis=0)
                    )
                    for i in range(units):
                        value = packet_ref[s, c, pl.ds(local[i], 1), :]
                        steps[i].append(
                            (value <= limit[i]).astype(jnp.float32).astype(jnp.bfloat16)
                        )
            weight = jnp.concatenate(weights, axis=1)
            step = jnp.concatenate([jnp.concatenate(p, axis=1) for p in steps], axis=0)
            product = lax.dot_general(
                weight, step, (((1,), (1,)), ((), ())), preferred_element_type=jnp.float32
            )
            return product, grad_sum, hess_sum

        flags = []
        for s0 in range(0, devices, 16):
            flag = jnp.zeros((1, LANES), jnp.float32)
            for s in range(s0, min(s0 + 16, devices)):
                row = plan["vote_lines"]
                count = packet_ref[s, chunks + row // plan["rows"], row % plan["rows"], :]
                flag = flag + jnp.where(
                    count.reshape(1, LANES) > float(half * LANES), float(1 << (s - s0)), 0.0
                )
            flags.append(jnp.max(flag).astype(jnp.int32))
        total, grad_all, hess_all = terms(range(chunk), range(half))
        for s0 in range(chunk, devices, chunk):
            more, grad_more, hess_more = terms(range(s0, s0 + chunk), range(half))
            total = total + more
            grad_all = grad_all + grad_more
            hess_all = hess_all + hess_more
        total_ref[...] = total
        grad_ref[...] = grad_all
        hess_ref[...] = hess_all
        for s0 in range(0, devices, 16):
            flag = flags[s0 // 16]

            def late(k, carry, s0=s0, flag=flag):
                @pl.when((jnp.right_shift(flag, k) & 1) == 1)
                def _():
                    more, grad_more, hess_more = terms([s0 + k], range(half, chunks))
                    total_ref[...] += more
                    grad_ref[...] += grad_more
                    hess_ref[...] += hess_more

                return carry

            lax.fori_loop(0, min(16, devices - s0), late, 0)
        total = total_ref[...]
        grad_all = grad_ref[...]
        hess_all = hess_ref[...]
        prefix_grad = total[0:leaves] + total[2 * leaves : 3 * leaves]
        prefix_hess = total[leaves : 2 * leaves] + total[3 * leaves :]
        whole_grad = jnp.sum(grad_all, axis=1, keepdims=True)
        whole_hess = jnp.sum(hess_all, axis=1, keepdims=True)
        rest_grad = whole_grad - prefix_grad
        rest_hess = whole_hess - prefix_hess
        gains = (
            prefix_grad * prefix_grad / (prefix_hess + ridge_weight)
            + rest_grad * rest_grad / (rest_hess + ridge_weight)
            - whole_grad * whole_grad / (whole_hess + ridge_weight)
        )
        for i in range(units):
            out_ref[i * leaves : (i + 1) * leaves, :] = gains[:, i * LANES : (i + 1) * LANES]

    vmem = pl.BlockSpec(memory_space=pltpu.VMEM)
    return pl.pallas_call(
        body,
        in_specs=[pl.BlockSpec(memory_space=pltpu.SMEM), vmem],
        out_specs=vmem,
        out_shape=vmem_array((units * leaves, LANES)),
        scratch_shapes=[
            pltpu.VMEM((4 * leaves, units * LANES), jnp.float32),
            pltpu.VMEM((leaves, LANES), jnp.float32),
            pltpu.VMEM((leaves, LANES), jnp.float32),
        ],
        compiler_params=pltpu.CompilerParams(vmem_limit_bytes=48 << 20),
        name="gain_stage",
    )(where, in_vmem(packets))


def vote_stage(packets, before, sources, features, leaves, kept, plan):
    rows = plan["rows"]
    lines = plan["vote_lines"]
    step = 64
    depth = round_up(features, LANES)
    last = before is not None

    def body(packet_ref, *refs):
        out_ref, count = refs[-2:] if last else (None, refs[-1])
        lane = lax.broadcasted_iota(jnp.int32, (1, LANES), 1)

        def block(index, carry):
            start = pl.multiple_of(index * step, step)
            feature = (lax.broadcasted_iota(jnp.int32, (step, LANES), 0) + start).astype(
                jnp.float32
            )
            total = jnp.zeros((step, LANES), jnp.float32)
            if last:
                total = refs[0][pl.ds(start, step), :]
            for s in sources:
                for line in range(lines):
                    row = line % rows
                    values = packet_ref[s, plan["chunks"] + line // rows, row : row + 1, :]
                    inside = kept * leaves - line * LANES
                    if inside < LANES:
                        values = jnp.where(lane < inside, values, -1.0)
                    total = total + (values == feature).astype(jnp.float32)
            count[pl.ds(start, step), :] = total
            return carry

        lax.fori_loop(0, depth // step, block, 0)
        if last:
            turned = count[...].T
            summed = turned[0:leaves]
            for i in range(1, LANES // leaves):
                summed = summed + turned[i * leaves : (i + 1) * leaves]
            out_ref[...] = summed[:, 0:features].astype(jnp.int32)

    vmem = pl.BlockSpec(memory_space=pltpu.VMEM)
    if last:
        inputs = [in_vmem(packets), in_vmem(before)]
        out_shape = jax.ShapeDtypeStruct((leaves, features), jnp.int32)
        scratch = [pltpu.VMEM((depth, LANES), jnp.float32)]
    else:
        inputs = [in_vmem(packets)]
        out_shape = vmem_array((depth, LANES))
        scratch = []
    return pl.pallas_call(
        body,
        in_specs=[vmem] * len(inputs),
        out_specs=vmem,
        out_shape=out_shape,
        scratch_shapes=scratch,
        compiler_params=pltpu.CompilerParams(vmem_limit_bytes=48 << 20),
        cost_estimate=pl.CostEstimate(flops=20_000_000, bytes_accessed=400_000, transcendentals=0),
        name="vote_stage",
    )(*inputs)


def place_stage(blocks, where, leaves, picked, plan):
    units = plan["units"]
    owners = plan["owners"]
    step = 8 if leaves % 8 == 0 else leaves

    rows = step * picked
    groups = leaves // step

    def body(where_ref, *refs):
        out_ref, planes, done = refs[-3:]
        here = where_ref[0] % owners
        odd = here & 1
        owner = []
        for index in range(len(blocks)):
            if not plan["doubling"]:
                owner.append(index)
                continue
            even_tag, odd_tag = plan["tags"][index % len(plan["tags"])]
            if index < len(plan["tags"]):
                owner.append(here ^ jnp.where(odd == 1, odd_tag, even_tag))
            else:
                owner.append(here ^ 1 ^ jnp.where(odd == 1, even_tag, odd_tag))
        copies = []
        for g in range(groups):
            for index, ref in enumerate(refs[:-3]):
                for i in range(units):

                    def write(index=index, ref=ref, i=i):
                        if units % HALVES == 0:
                            half = i % HALVES
                            pick = owner[index] * (units // HALVES) + i // HALVES
                        else:
                            half = (owner[index] * units + i) % HALVES
                            pick = (owner[index] * units + i) // HALVES
                        start = i * leaves + g * step
                        planes[half, pl.ds(g * rows + pick, step, stride=picked), :] = ref[
                            start : start + step, :
                        ]

                    if owners * units == picked * HALVES:
                        write()
                    else:
                        pl.when(owner[index] * units + i < picked * HALVES)(write)
            for half in range(HALVES):
                copy = pltpu.make_async_copy(
                    planes.at[half, pl.ds(g * rows, rows), :],
                    out_ref.at[pl.ds(g * rows, rows), pl.ds(half * LANES, LANES)],
                    done.at[g * HALVES + half],
                )
                copy.start()
                copies.append(copy)
        for copy in copies:
            copy.wait()

    vmem = pl.BlockSpec(memory_space=pltpu.VMEM)
    return pl.pallas_call(
        body,
        in_specs=[pl.BlockSpec(memory_space=pltpu.SMEM)] + [vmem] * len(blocks),
        out_specs=pl.BlockSpec(memory_space=pltpu.HBM),
        out_shape=jax.ShapeDtypeStruct((leaves * picked, B), jnp.float32),
        scratch_shapes=[
            pltpu.VMEM((HALVES, leaves * picked, LANES), jnp.float32),
            pltpu.SemaphoreType.DMA((groups * HALVES,)),
        ],
        compiler_params=pltpu.CompilerParams(vmem_limit_bytes=48 << 20),
        name="place_stage",
    )(where, *[in_vmem(b) for b in blocks]).reshape(leaves, picked, B)


def solution(mesh):
    devices = mesh.shape["rows"]

    def on_device(
        feature_bin, doc_leaf, current_score, relevance, doc_rank, query_length, feature_votes,
        elected,
    ):
        documents, features = feature_bin.shape
        leaves, picked = elected.shape
        kept = feature_votes.shape[2]
        doubling = devices >= 8 and devices & (devices - 1) == 0
        owners = devices // 2 if doubling else devices
        units = cdiv(picked * HALVES, owners)
        padded = round_up(picked, 8)
        picks = max(
            (j * units + units - 1) // HALVES - (j * units) // HALVES + 1 for j in range(owners)
        )
        rows = round_up(picks + 3, 8)
        plan = {
            "devices": devices,
            "doubling": doubling,
            "owners": owners,
            "units": units,
            "picks": picks,
            "padded": padded,
            "first": [min(j * units // HALVES, padded - picks) for j in range(owners)],
            "rows": rows,
            "chunks": documents // LANES,
            "vote_lines": cdiv(kept * leaves, LANES),
            "vote_tiles": cdiv(cdiv(kept * leaves, LANES) + 1, rows),
        }
        where = lax.axis_index("rows").astype(jnp.int32).reshape(1)
        gradient, hessian, packets = local_stage(
            feature_bin.T,
            doc_leaf.reshape(1, -1),
            current_score.reshape(1, -1),
            relevance.reshape(1, -1),
            doc_rank.reshape(1, -1),
            query_length,
            feature_votes.transpose(2, 0, 1),
            elected,
            plan,
        )
        received = lax.all_to_all(packets, "rows", 0, 0)
        block = gain_stage(received, where, leaves, plan)
        middle = cdiv(devices, 2)
        count_args = (features, leaves, kept, plan)
        votes = vote_stage(received, None, range(middle), *count_args)
        if doubling:
            far = [1 << b for b in reversed(range(1, owners.bit_length() - 1))]
            twin = list(far)
            twin[-2:] = twin[-2:][::-1]
            pairs = [
                [(i, i ^ (twin[p] if i & 1 else far[p])) for i in range(devices)]
                for p in range(len(far))
            ]
            blocks = [block]
            tags = [(0, 0)]
            for p in range(len(far)):
                moved = [lax.ppermute(b, "rows", pairs[p]) for b in blocks]
                if p == len(far) - 1:
                    votes = vote_stage(received, votes, range(middle, devices), *count_args)
                    moved[-1], votes = lax.optimization_barrier((moved[-1], votes))
                elif p == len(far) - 2:
                    moved[0], votes = lax.optimization_barrier((moved[0], votes))
                blocks = blocks + moved
                tags = tags + [(even | far[p], odd | twin[p]) for even, odd in tags]
            sibling = [(i, i ^ 1) for i in range(devices)]
            blocks = blocks + [lax.ppermute(b, "rows", sibling) for b in blocks]
            plan["tags"] = tags
        else:
            votes = vote_stage(received, votes, range(middle, devices), *count_args)
            gathered = lax.all_gather(block, "rows", axis=0)
            blocks = [gathered[j] for j in range(devices)]
            plan["tags"] = None
        split_gain = place_stage(blocks, where, leaves, picked, plan)
        return gradient.reshape(-1), hessian.reshape(-1), votes, split_gain

    return jax.shard_map(
        on_device,
        mesh=mesh,
        in_specs=(
            P(("parts", "rows"), None),
            P(("parts", "rows")),
            P(("parts", "rows")),
            P(("parts", "rows")),
            P(("parts", "rows")),
            P(("parts", "rows")),
            P(("parts", "rows"), None, None),
            P("parts", None),
        ),
        out_specs=(
            P(("parts", "rows")),
            P(("parts", "rows")),
            P("parts", None),
            P("parts", None, None),
        ),
        check_vma=False,
    )
```

```python
import jax
import jax.numpy as jnp
from jax import lax
from jax.experimental import pallas as pl
from jax.experimental.pallas import tpu as pltpu
from jax.sharding import PartitionSpec as P

B = 256
LANES = 128
HALVES = B // LANES
LEVELS = 4

ridge_weight = 1.0


def cdiv(a, b):
    return -(-a // b)


def round_up(a, b):
    return cdiv(a, b) * b


def query_rows(score, level, rank, lengths, slots):
    documents = score.shape[1]
    queries = documents // slots
    gain = jnp.left_shift(1, level).astype(jnp.float32) - 1.0
    discount = 1.0 / jnp.log2(rank.astype(jnp.float32) + 2.0)
    place = lax.broadcasted_iota(jnp.int32, (1, slots), 1)
    place_discount = 1.0 / jnp.log2(place.astype(jnp.float32) + 2.0)
    gradients = []
    hessians = []
    for q in range(queries):
        lanes = slice(q * slots, (q + 1) * slots)
        live = place < lengths[q]
        live_row = live.astype(jnp.float32)
        score_row = score[:, lanes]
        gain_row = gain[:, lanes]
        discount_row = discount[:, lanes]
        level_row = jnp.where(live, level[:, lanes], -1)
        ideal_gain = jnp.zeros((1, slots), jnp.float32)
        for v in range(1, LEVELS + 1):
            count = jnp.sum((level_row >= v).astype(jnp.float32), axis=1, keepdims=True)
            ideal_gain = ideal_gain + jnp.where(
                place.astype(jnp.float32) < count, float(2 ** (v - 1)), 0.0
            )
        ideal = jnp.sum(ideal_gain * place_discount, axis=1, keepdims=True)
        scaling = 1.0 / jnp.maximum(ideal, 1.0)
        rows = jnp.concatenate(
            [score_row, gain_row, discount_row, live_row, jnp.zeros((4, slots), jnp.float32)],
            axis=0,
        )
        columns = rows.T
        step = 32
        push_sum = jnp.zeros((8, slots), jnp.float32)
        curve_sum = jnp.zeros((8, slots), jnp.float32)
        for r in range(0, slots, step):
            part = columns[r : r + step]
            gap = (part[:, 1:2] - gain_row) * part[:, 3:4]
            change = gap * jnp.abs(part[:, 2:3] - discount_row)
            lead = score_row - part[:, 0:1]
            chance = 1.0 / (1.0 + jnp.exp(jnp.where(gap > 0.0, -lead, lead)))
            push = chance * change
            curve = (1.0 - chance) * jnp.abs(push)
            for k in range(0, step, 8):
                push_sum = push_sum + push[k : k + 8]
                curve_sum = curve_sum + curve[k : k + 8]
        factor = scaling * live_row
        gradients.append(jnp.sum(push_sum, axis=0, keepdims=True) * factor)
        hessians.append(jnp.sum(curve_sum, axis=0, keepdims=True) * factor)
    return jnp.concatenate(gradients, axis=1), jnp.concatenate(hessians, axis=1)


def vmem_array(shape):
    return pltpu.VMEM(shape, jnp.float32)


def in_vmem(x):
    return pltpu.with_memory_space_constraint(x, pltpu.VMEM)


def in_hbm(x):
    return pltpu.with_memory_space_constraint(x, pltpu.HBM)


def local_stage(bins, leaf, score, level, rank, lengths, votes, elected, plan):
    features, documents = bins.shape
    leaves, picked = elected.shape
    kept = votes.shape[0]
    padded = plan["padded"]
    picks = plan["picks"]
    rows = plan["rows"]
    slots = documents // lengths.shape[0]
    group = 8 if leaves % 8 == 0 else leaves
    per_row = LANES // leaves

    piece = round_up(cdiv(features, 4), 8)
    cuts = [(f, min(piece, features - f)) for f in range(0, features, piece)]

    def body(*refs):
        sources = refs[0:8]
        grad_ref, hess_ref, packet_ref = refs[8:11]
        square, chosen_ref = refs[11:13]
        copied = refs[13:21]
        arrived = refs[21]
        bins_here, leaf_ref, score_ref, level_ref, rank_ref, length_ref, votes_ref, elected_ref = (
            copied
        )
        small = [
            pltpu.make_async_copy(sources[k], copied[k], arrived.at[len(cuts) + k - 1])
            for k in (5, 2, 3, 4, 7, 1, 6)
        ]
        fetches = [
            pltpu.make_async_copy(
                sources[0].at[pl.ds(f, size), :], bins_here.at[pl.ds(f, size), :], arrived.at[k]
            )
            for k, (f, size) in enumerate(cuts)
        ]
        for copy in small + fetches:
            copy.start()
        for copy in small:
            copy.wait()
        square[...] = jnp.zeros(square.shape, jnp.float32)
        square[0:leaves, 0:picked] = elected_ref[...].astype(jnp.float32)
        elected_t = square[...].T
        leaf_row = leaf_ref[...]
        gradient, hessian = query_rows(
            score_ref[...], level_ref[...], rank_ref[...], length_ref, slots
        )
        grad_ref[...] = gradient
        hess_ref[...] = hessian
        lane = lax.broadcasted_iota(jnp.int32, (1, documents), 1)
        starts = [0]
        for q in range(documents // slots):
            starts.append(starts[-1] + length_ref[q])

        def compact(block):
            result = block
            for q in range(1, documents // slots):
                moved = pltpu.roll(block, starts[q] - q * slots + documents, 1)
                result = jnp.where(lane >= starts[q], moved, result)
            return result

        shared = [leaf_row.astype(jnp.float32), gradient, hessian]
        shared.append(jnp.zeros((max(rows - picks, 8) - 3, documents), jnp.float32))
        shared = compact(jnp.concatenate(shared, axis=0))[0 : rows - picks]
        shared = jnp.where(lane < starts[-1], shared, 0.0)
        count = jnp.zeros((1, LANES), jnp.float32) + starts[-1].astype(jnp.float32)
        for fetch in fetches:
            fetch.wait()
        table = bins_here[...].astype(jnp.float32).astype(jnp.bfloat16)
        feature = lax.broadcasted_iota(jnp.int32, (padded, features), 1).astype(jnp.float32)
        chosen = jnp.zeros((padded, documents), jnp.float32)
        for first in range(0, leaves, group):
            hot = []
            for l in range(first, first + group):
                hot.append((elected_t[0:padded, l : l + 1] == feature).astype(jnp.float32))
            hot = jnp.concatenate(hot, axis=0).astype(jnp.bfloat16)
            found = jnp.dot(hot, table, preferred_element_type=jnp.float32)
            for i in range(group):
                chosen = jnp.where(
                    leaf_row == first + i, found[i * padded : (i + 1) * padded], chosen
                )
        chosen_ref[...] = compact(chosen)
        tail = []
        for k0 in range(0, kept, per_row):
            line = jnp.zeros((1, LANES), jnp.float32)
            for i in range(min(per_row, kept - k0)):
                values = votes_ref[k0 + i].astype(jnp.float32)
                pieces = [values]
                if i:
                    pieces.insert(0, jnp.zeros((1, i * leaves), jnp.float32))
                if (i + 1) * leaves < LANES:
                    pieces.append(jnp.zeros((1, LANES - (i + 1) * leaves), jnp.float32))
                line = line + jnp.concatenate(pieces, axis=1)
            tail.append(line)
        tail.append(count)
        spare = plan["vote_tiles"] * rows - len(tail)
        if spare:
            tail.append(jnp.zeros((spare, LANES), jnp.float32))
        tail = jnp.concatenate(tail, axis=0)
        for j in range(plan["devices"]):
            start = plan["first"][j % plan["owners"]]
            block = jnp.concatenate([chosen_ref[start : start + picks, :], shared], axis=0)
            for c in range(documents // LANES):
                packet_ref[j, c] = block[:, c * LANES : (c + 1) * LANES]
            for t in range(plan["vote_tiles"]):
                packet_ref[j, documents // LANES + t] = tail[t * rows : (t + 1) * rows]

    vmem = pl.BlockSpec(memory_space=pltpu.VMEM)
    return pl.pallas_call(
        body,
        in_specs=[pl.BlockSpec(memory_space=pltpu.HBM)] * 8,
        out_specs=[vmem] * 3,
        out_shape=[
            jax.ShapeDtypeStruct((1, documents), jnp.float32),
            jax.ShapeDtypeStruct((1, documents), jnp.float32),
            vmem_array(
                (plan["devices"], documents // LANES + plan["vote_tiles"], rows, LANES)
            ),
        ],
        scratch_shapes=[
            pltpu.VMEM((LANES, LANES), jnp.float32),
            pltpu.VMEM((padded, documents), jnp.float32),
            pltpu.VMEM((features, documents), jnp.int32),
            pltpu.VMEM((1, documents), jnp.int32),
            pltpu.VMEM((1, documents), jnp.float32),
            pltpu.VMEM((1, documents), jnp.int32),
            pltpu.VMEM((1, documents), jnp.int32),
            pltpu.SMEM(lengths.shape, jnp.int32),
            pltpu.VMEM(votes.shape, jnp.int32),
            pltpu.VMEM(elected.shape, jnp.int32),
            pltpu.SemaphoreType.DMA((len(cuts) + 7,)),
        ],
        compiler_params=pltpu.CompilerParams(vmem_limit_bytes=48 << 20),
        name="local_stage",
    )(*[in_hbm(x) for x in (bins, leaf, score, level, rank, lengths, votes, elected)])


def gain_stage(packets, where, leaves, plan):
    devices = packets.shape[0]
    picks = plan["picks"]
    units = plan["units"]
    chunks = plan["chunks"]
    chunk = 4 if devices % 4 == 0 else 1
    even = units % HALVES == 0

    half = cdiv(chunks, 2)

    def body(where_ref, packet_ref, out_ref, total_ref, grad_ref, hess_ref, late_ref):
        leaf_id = lax.broadcasted_iota(jnp.int32, (leaves, LANES), 0).astype(jnp.float32)
        bin_id = lax.broadcasted_iota(jnp.int32, (LANES, LANES), 0).astype(jnp.float32)
        local = []
        limit = []
        base = where_ref[0] % plan["owners"] * units
        first = jnp.minimum(base // HALVES, plan["padded"] - picks)
        for i in range(units):
            if even:
                local.append(i // HALVES)
                limit.append(bin_id + float(i % HALVES * LANES))
            else:
                local.append(jnp.clip((base + i) // HALVES - first, 0, picks - 1))
                limit.append(bin_id + ((base + i) % HALVES * LANES).astype(jnp.float32))
        def terms(sources, parts):
            weights = []
            steps = [[] for _ in range(units)]
            grad_sum = jnp.zeros((leaves, LANES), jnp.float32)
            hess_sum = jnp.zeros((leaves, LANES), jnp.float32)
            for s in sources:
                for c in parts:
                    mine = packet_ref[s, c, picks : picks + 1, :] == leaf_id
                    grad = jnp.where(mine, packet_ref[s, c, picks + 1 : picks + 2, :], 0.0)
                    hess = jnp.where(mine, packet_ref[s, c, picks + 2 : picks + 3, :], 0.0)
                    grad_sum = grad_sum + grad
                    hess_sum = hess_sum + hess
                    grad_high = grad.astype(jnp.bfloat16)
                    hess_high = hess.astype(jnp.bfloat16)
                    grad_low = (grad - grad_high.astype(jnp.float32)).astype(jnp.bfloat16)
                    hess_low = (hess - hess_high.astype(jnp.float32)).astype(jnp.bfloat16)
                    weights.append(
                        jnp.concatenate([grad_high, hess_high, grad_low, hess_low], axis=0)
                    )
                    for i in range(units):
                        value = packet_ref[s, c, pl.ds(local[i], 1), :]
                        steps[i].append(
                            (value <= limit[i]).astype(jnp.float32).astype(jnp.bfloat16)
                        )
            weight = jnp.concatenate(weights, axis=1)
            step = jnp.concatenate([jnp.concatenate(p, axis=1) for p in steps], axis=0)
            product = lax.dot_general(
                weight, step, (((1,), (1,)), ((), ())), preferred_element_type=jnp.float32
            )
            return product, grad_sum, hess_sum

        flags = []
        for s0 in range(0, devices, 16):
            flag = jnp.zeros((1, LANES), jnp.float32)
            for s in range(s0, min(s0 + 16, devices)):
                row = plan["vote_lines"]
                count = packet_ref[s, chunks + row // plan["rows"], row % plan["rows"], :]
                flag = flag + jnp.where(
                    count.reshape(1, LANES) > float(half * LANES), float(1 << (s - s0)), 0.0
                )
            flags.append(jnp.max(flag).astype(jnp.int32))
        total, grad_all, hess_all = terms(range(chunk), range(half))
        for s0 in range(chunk, devices, chunk):
            more, grad_more, hess_more = terms(range(s0, s0 + chunk), range(half))
            total = total + more
            grad_all = grad_all + grad_more
            hess_all = hess_all + hess_more
        total_ref[...] = total
        grad_ref[...] = grad_all
        hess_ref[...] = hess_all
        late = jnp.int32(0)
        for s in range(devices):
            late_ref[late] = s
            late = late + (jnp.right_shift(flags[s // 16], s % 16) & 1)

        def add(k, carry):
            more, grad_more, hess_more = terms([late_ref[k]], range(half, chunks))
            total_ref[...] += more
            grad_ref[...] += grad_more
            hess_ref[...] += hess_more
            return carry

        lax.fori_loop(0, late, add, 0)
        total = total_ref[...]
        grad_all = grad_ref[...]
        hess_all = hess_ref[...]
        prefix_grad = total[0:leaves] + total[2 * leaves : 3 * leaves]
        prefix_hess = total[leaves : 2 * leaves] + total[3 * leaves :]
        whole_grad = jnp.sum(grad_all, axis=1, keepdims=True)
        whole_hess = jnp.sum(hess_all, axis=1, keepdims=True)
        rest_grad = whole_grad - prefix_grad
        rest_hess = whole_hess - prefix_hess
        gains = (
            prefix_grad * prefix_grad / (prefix_hess + ridge_weight)
            + rest_grad * rest_grad / (rest_hess + ridge_weight)
            - whole_grad * whole_grad / (whole_hess + ridge_weight)
        )
        for i in range(units):
            out_ref[i * leaves : (i + 1) * leaves, :] = gains[:, i * LANES : (i + 1) * LANES]

    vmem = pl.BlockSpec(memory_space=pltpu.VMEM)
    return pl.pallas_call(
        body,
        in_specs=[pl.BlockSpec(memory_space=pltpu.SMEM), vmem],
        out_specs=vmem,
        out_shape=vmem_array((units * leaves, LANES)),
        scratch_shapes=[
            pltpu.VMEM((4 * leaves, units * LANES), jnp.float32),
            pltpu.VMEM((leaves, LANES), jnp.float32),
            pltpu.VMEM((leaves, LANES), jnp.float32),
            pltpu.SMEM((devices + 1,), jnp.int32),
        ],
        compiler_params=pltpu.CompilerParams(vmem_limit_bytes=48 << 20),
        name="gain_stage",
    )(where, in_vmem(packets))


def vote_stage(packets, before, sources, features, leaves, kept, plan):
    rows = plan["rows"]
    lines = plan["vote_lines"]
    step = 64
    depth = round_up(features, LANES)
    last = before is not None

    def body(packet_ref, *refs):
        out_ref, count = refs[-2:] if last else (None, refs[-1])
        lane = lax.broadcasted_iota(jnp.int32, (1, LANES), 1)

        def block(index, carry):
            start = pl.multiple_of(index * step, step)
            feature = (lax.broadcasted_iota(jnp.int32, (step, LANES), 0) + start).astype(
                jnp.float32
            )
            total = jnp.zeros((step, LANES), jnp.float32)
            if last:
                total = refs[0][pl.ds(start, step), :]
            for s in sources:
                for line in range(lines):
                    row = line % rows
                    values = packet_ref[s, plan["chunks"] + line // rows, row : row + 1, :]
                    inside = kept * leaves - line * LANES
                    if inside < LANES:
                        values = jnp.where(lane < inside, values, -1.0)
                    total = total + (values == feature).astype(jnp.float32)
            count[pl.ds(start, step), :] = total
            return carry

        lax.fori_loop(0, depth // step, block, 0)
        if last:
            turned = count[...].T
            summed = turned[0:leaves]
            for i in range(1, LANES // leaves):
                summed = summed + turned[i * leaves : (i + 1) * leaves]
            out_ref[...] = summed[:, 0:features].astype(jnp.int32)

    vmem = pl.BlockSpec(memory_space=pltpu.VMEM)
    if last:
        inputs = [in_vmem(packets), in_vmem(before)]
        out_shape = jax.ShapeDtypeStruct((leaves, features), jnp.int32)
        scratch = [pltpu.VMEM((depth, LANES), jnp.float32)]
    else:
        inputs = [in_vmem(packets)]
        out_shape = vmem_array((depth, LANES))
        scratch = []
    return pl.pallas_call(
        body,
        in_specs=[vmem] * len(inputs),
        out_specs=vmem,
        out_shape=out_shape,
        scratch_shapes=scratch,
        compiler_params=pltpu.CompilerParams(vmem_limit_bytes=48 << 20),
        cost_estimate=pl.CostEstimate(flops=20_000_000, bytes_accessed=400_000, transcendentals=0),
        name="vote_stage",
    )(*inputs)


def place_stage(blocks, where, leaves, picked, plan):
    units = plan["units"]
    owners = plan["owners"]
    step = 8 if leaves % 8 == 0 else leaves

    rows = step * picked
    groups = leaves // step

    def body(where_ref, *refs):
        out_ref, planes, done = refs[-3:]
        here = where_ref[0] % owners
        odd = here & 1
        owner = []
        for index in range(len(blocks)):
            if not plan["doubling"]:
                owner.append(index)
                continue
            even_tag, odd_tag = plan["tags"][index % len(plan["tags"])]
            if index < len(plan["tags"]):
                owner.append(here ^ jnp.where(odd == 1, odd_tag, even_tag))
            else:
                owner.append(here ^ 1 ^ jnp.where(odd == 1, even_tag, odd_tag))
        copies = []
        for g in range(groups):
            for index, ref in enumerate(refs[:-3]):
                for i in range(units):

                    def write(index=index, ref=ref, i=i):
                        if units % HALVES == 0:
                            half = i % HALVES
                            pick = owner[index] * (units // HALVES) + i // HALVES
                        else:
                            half = (owner[index] * units + i) % HALVES
                            pick = (owner[index] * units + i) // HALVES
                        start = i * leaves + g * step
                        planes[half, pl.ds(g * rows + pick, step, stride=picked), :] = ref[
                            start : start + step, :
                        ]

                    if owners * units == picked * HALVES:
                        write()
                    else:
                        pl.when(owner[index] * units + i < picked * HALVES)(write)
            for half in range(HALVES):
                copy = pltpu.make_async_copy(
                    planes.at[half, pl.ds(g * rows, rows), :],
                    out_ref.at[pl.ds(g * rows, rows), pl.ds(half * LANES, LANES)],
                    done.at[g * HALVES + half],
                )
                copy.start()
                copies.append(copy)
        for copy in copies:
            copy.wait()

    vmem = pl.BlockSpec(memory_space=pltpu.VMEM)
    return pl.pallas_call(
        body,
        in_specs=[pl.BlockSpec(memory_space=pltpu.SMEM)] + [vmem] * len(blocks),
        out_specs=pl.BlockSpec(memory_space=pltpu.HBM),
        out_shape=jax.ShapeDtypeStruct((leaves * picked, B), jnp.float32),
        scratch_shapes=[
            pltpu.VMEM((HALVES, leaves * picked, LANES), jnp.float32),
            pltpu.SemaphoreType.DMA((groups * HALVES,)),
        ],
        compiler_params=pltpu.CompilerParams(vmem_limit_bytes=48 << 20),
        name="place_stage",
    )(where, *[in_vmem(b) for b in blocks]).reshape(leaves, picked, B)


def solution(mesh):
    devices = mesh.shape["rows"]

    def on_device(
        feature_bin, doc_leaf, current_score, relevance, doc_rank, query_length, feature_votes,
        elected,
    ):
        documents, features = feature_bin.shape
        leaves, picked = elected.shape
        kept = feature_votes.shape[2]
        doubling = devices >= 8 and devices & (devices - 1) == 0
        owners = devices // 2 if doubling else devices
        units = cdiv(picked * HALVES, owners)
        padded = round_up(picked, 8)
        picks = max(
            (j * units + units - 1) // HALVES - (j * units) // HALVES + 1 for j in range(owners)
        )
        rows = round_up(picks + 3, 8)
        plan = {
            "devices": devices,
            "doubling": doubling,
            "owners": owners,
            "units": units,
            "picks": picks,
            "padded": padded,
            "first": [min(j * units // HALVES, padded - picks) for j in range(owners)],
            "rows": rows,
            "chunks": documents // LANES,
            "vote_lines": cdiv(kept * leaves, LANES),
            "vote_tiles": cdiv(cdiv(kept * leaves, LANES) + 1, rows),
        }
        where = lax.axis_index("rows").astype(jnp.int32).reshape(1)
        gradient, hessian, packets = local_stage(
            feature_bin.T,
            doc_leaf.reshape(1, -1),
            current_score.reshape(1, -1),
            relevance.reshape(1, -1),
            doc_rank.reshape(1, -1),
            query_length,
            feature_votes.transpose(2, 0, 1),
            elected,
            plan,
        )
        received = lax.all_to_all(packets, "rows", 0, 0)
        block = gain_stage(received, where, leaves, plan)
        middle = cdiv(devices, 2)
        count_args = (features, leaves, kept, plan)
        votes = vote_stage(received, None, range(middle), *count_args)
        if doubling:
            far = [1 << b for b in reversed(range(1, owners.bit_length() - 1))]
            twin = list(far)
            twin[-2:] = twin[-2:][::-1]
            pairs = [
                [(i, i ^ (twin[p] if i & 1 else far[p])) for i in range(devices)]
                for p in range(len(far))
            ]
            blocks = [block]
            tags = [(0, 0)]
            for p in range(len(far)):
                moved = [lax.ppermute(b, "rows", pairs[p]) for b in blocks]
                if p == len(far) - 1:
                    votes = vote_stage(received, votes, range(middle, devices), *count_args)
                    moved[-1], votes = lax.optimization_barrier((moved[-1], votes))
                elif p == len(far) - 2:
                    moved[0], votes = lax.optimization_barrier((moved[0], votes))
                blocks = blocks + moved
                tags = tags + [(even | far[p], odd | twin[p]) for even, odd in tags]
            sibling = [(i, i ^ 1) for i in range(devices)]
            blocks = blocks + [lax.ppermute(b, "rows", sibling) for b in blocks]
            plan["tags"] = tags
        else:
            votes = vote_stage(received, votes, range(middle, devices), *count_args)
            gathered = lax.all_gather(block, "rows", axis=0)
            blocks = [gathered[j] for j in range(devices)]
            plan["tags"] = None
        split_gain = place_stage(blocks, where, leaves, picked, plan)
        return gradient.reshape(-1), hessian.reshape(-1), votes, split_gain

    return jax.shard_map(
        on_device,
        mesh=mesh,
        in_specs=(
            P(("parts", "rows"), None),
            P(("parts", "rows")),
            P(("parts", "rows")),
            P(("parts", "rows")),
            P(("parts", "rows")),
            P(("parts", "rows")),
            P(("parts", "rows"), None, None),
            P("parts", None),
        ),
        out_specs=(
            P(("parts", "rows")),
            P(("parts", "rows")),
            P("parts", None),
            P("parts", None, None),
        ),
        check_vma=False,
    )
```

```python
import jax
import jax.numpy as jnp
from jax import lax
from jax.experimental import pallas as pl
from jax.experimental.pallas import tpu as pltpu
from jax.sharding import PartitionSpec as P

B = 256
LANES = 128
HALVES = B // LANES
LEVELS = 4

ridge_weight = 1.0


def cdiv(a, b):
    return -(-a // b)


def round_up(a, b):
    return cdiv(a, b) * b


def query_rows(score, level, rank, lengths, slots):
    documents = score.shape[1]
    queries = documents // slots
    gain = jnp.left_shift(1, level).astype(jnp.float32) - 1.0
    discount = 1.0 / jnp.log2(rank.astype(jnp.float32) + 2.0)
    place = lax.broadcasted_iota(jnp.int32, (1, slots), 1)
    place_discount = 1.0 / jnp.log2(place.astype(jnp.float32) + 2.0)
    gradients = []
    hessians = []
    for q in range(queries):
        lanes = slice(q * slots, (q + 1) * slots)
        live = place < lengths[q]
        live_row = live.astype(jnp.float32)
        score_row = score[:, lanes]
        gain_row = gain[:, lanes]
        discount_row = discount[:, lanes]
        level_row = jnp.where(live, level[:, lanes], -1)
        ideal_gain = jnp.zeros((1, slots), jnp.float32)
        for v in range(1, LEVELS + 1):
            count = jnp.sum((level_row >= v).astype(jnp.float32), axis=1, keepdims=True)
            ideal_gain = ideal_gain + jnp.where(
                place.astype(jnp.float32) < count, float(2 ** (v - 1)), 0.0
            )
        ideal = jnp.sum(ideal_gain * place_discount, axis=1, keepdims=True)
        scaling = 1.0 / jnp.maximum(ideal, 1.0)
        rows = jnp.concatenate(
            [score_row, gain_row, discount_row, live_row, jnp.zeros((4, slots), jnp.float32)],
            axis=0,
        )
        columns = rows.T
        step = 32
        push_sum = jnp.zeros((8, slots), jnp.float32)
        curve_sum = jnp.zeros((8, slots), jnp.float32)
        for r in range(0, slots, step):
            part = columns[r : r + step]
            gap = (part[:, 1:2] - gain_row) * part[:, 3:4]
            change = gap * jnp.abs(part[:, 2:3] - discount_row)
            lead = score_row - part[:, 0:1]
            chance = 1.0 / (1.0 + jnp.exp(jnp.where(gap > 0.0, -lead, lead)))
            push = chance * change
            curve = (1.0 - chance) * jnp.abs(push)
            for k in range(0, step, 8):
                push_sum = push_sum + push[k : k + 8]
                curve_sum = curve_sum + curve[k : k + 8]
        factor = scaling * live_row
        gradients.append(jnp.sum(push_sum, axis=0, keepdims=True) * factor)
        hessians.append(jnp.sum(curve_sum, axis=0, keepdims=True) * factor)
    return jnp.concatenate(gradients, axis=1), jnp.concatenate(hessians, axis=1)


def vmem_array(shape):
    return pltpu.VMEM(shape, jnp.float32)


def in_vmem(x):
    return pltpu.with_memory_space_constraint(x, pltpu.VMEM)


def in_hbm(x):
    return pltpu.with_memory_space_constraint(x, pltpu.HBM)


def local_stage(bins, leaf, score, level, rank, lengths, votes, elected, plan):
    features, documents = bins.shape
    leaves, picked = elected.shape
    kept = votes.shape[0]
    padded = plan["padded"]
    picks = plan["picks"]
    rows = plan["rows"]
    slots = documents // lengths.shape[0]
    group = 8 if leaves % 8 == 0 else leaves
    per_row = LANES // leaves

    piece = round_up(cdiv(features, 4), 8)
    cuts = [(f, min(piece, features - f)) for f in range(0, features, piece)]

    def body(*refs):
        sources = refs[0:8]
        grad_ref, hess_ref, packet_ref = refs[8:11]
        square, chosen_ref = refs[11:13]
        copied = refs[13:21]
        arrived, hot_ref = refs[21:23]
        bins_here, leaf_ref, score_ref, level_ref, rank_ref, length_ref, votes_ref, elected_ref = (
            copied
        )
        small = [
            pltpu.make_async_copy(sources[k], copied[k], arrived.at[len(cuts) + k - 1])
            for k in (5, 2, 3, 4, 7, 1, 6)
        ]
        fetches = [
            pltpu.make_async_copy(
                sources[0].at[pl.ds(f, size), :], bins_here.at[pl.ds(f, size), :], arrived.at[k]
            )
            for k, (f, size) in enumerate(cuts)
        ]
        for copy in small + fetches:
            copy.start()
        for copy in small:
            copy.wait()
        square[...] = jnp.zeros(square.shape, jnp.float32)
        square[0:leaves, 0:picked] = elected_ref[...].astype(jnp.float32)
        elected_t = square[...].T
        leaf_row = leaf_ref[...]
        gradient, hessian = query_rows(
            score_ref[...], level_ref[...], rank_ref[...], length_ref, slots
        )
        grad_ref[...] = gradient
        hess_ref[...] = hessian
        lane = lax.broadcasted_iota(jnp.int32, (1, documents), 1)
        starts = [0]
        for q in range(documents // slots):
            starts.append(starts[-1] + length_ref[q])

        def compact(block):
            result = block
            for q in range(1, documents // slots):
                moved = pltpu.roll(block, starts[q] - q * slots + documents, 1)
                result = jnp.where(lane >= starts[q], moved, result)
            return result

        shared = [leaf_row.astype(jnp.float32), gradient, hessian]
        shared.append(jnp.zeros((max(rows - picks, 8) - 3, documents), jnp.float32))
        shared = compact(jnp.concatenate(shared, axis=0))[0 : rows - picks]
        shared = jnp.where(lane < starts[-1], shared, 0.0)
        count = jnp.zeros((1, LANES), jnp.float32) + starts[-1].astype(jnp.float32)
        feature = lax.broadcasted_iota(jnp.int32, (padded, features), 1).astype(jnp.float32)
        for first in range(0, leaves, group):
            hot = []
            for l in range(first, first + group):
                hot.append((elected_t[0:padded, l : l + 1] == feature).astype(jnp.float32))
            hot_ref[first * padded : (first + group) * padded, :] = jnp.concatenate(
                hot, axis=0
            ).astype(jnp.bfloat16)
        for fetch in fetches:
            fetch.wait()
        table = bins_here[...].astype(jnp.float32).astype(jnp.bfloat16)
        chosen = jnp.zeros((padded, documents), jnp.float32)
        for first in range(0, leaves, group):
            hot = hot_ref[first * padded : (first + group) * padded, :]
            found = jnp.dot(hot, table, preferred_element_type=jnp.float32)
            for i in range(group):
                chosen = jnp.where(
                    leaf_row == first + i, found[i * padded : (i + 1) * padded], chosen
                )
        chosen_ref[...] = compact(chosen)
        tail = []
        for k0 in range(0, kept, per_row):
            line = jnp.zeros((1, LANES), jnp.float32)
            for i in range(min(per_row, kept - k0)):
                values = votes_ref[k0 + i].astype(jnp.float32)
                pieces = [values]
                if i:
                    pieces.insert(0, jnp.zeros((1, i * leaves), jnp.float32))
                if (i + 1) * leaves < LANES:
                    pieces.append(jnp.zeros((1, LANES - (i + 1) * leaves), jnp.float32))
                line = line + jnp.concatenate(pieces, axis=1)
            tail.append(line)
        tail.append(count)
        spare = plan["vote_tiles"] * rows - len(tail)
        if spare:
            tail.append(jnp.zeros((spare, LANES), jnp.float32))
        tail = jnp.concatenate(tail, axis=0)
        for j in range(plan["devices"]):
            start = plan["first"][j % plan["owners"]]
            block = jnp.concatenate([chosen_ref[start : start + picks, :], shared], axis=0)
            for c in range(documents // LANES):
                packet_ref[j, c] = block[:, c * LANES : (c + 1) * LANES]
            for t in range(plan["vote_tiles"]):
                packet_ref[j, documents // LANES + t] = tail[t * rows : (t + 1) * rows]

    vmem = pl.BlockSpec(memory_space=pltpu.VMEM)
    return pl.pallas_call(
        body,
        in_specs=[pl.BlockSpec(memory_space=pltpu.HBM)] * 8,
        out_specs=[vmem] * 3,
        out_shape=[
            jax.ShapeDtypeStruct((1, documents), jnp.float32),
            jax.ShapeDtypeStruct((1, documents), jnp.float32),
            vmem_array(
                (plan["devices"], documents // LANES + plan["vote_tiles"], rows, LANES)
            ),
        ],
        scratch_shapes=[
            pltpu.VMEM((LANES, LANES), jnp.float32),
            pltpu.VMEM((padded, documents), jnp.float32),
            pltpu.VMEM((features, documents), jnp.int32),
            pltpu.VMEM((1, documents), jnp.int32),
            pltpu.VMEM((1, documents), jnp.float32),
            pltpu.VMEM((1, documents), jnp.int32),
            pltpu.VMEM((1, documents), jnp.int32),
            pltpu.SMEM(lengths.shape, jnp.int32),
            pltpu.VMEM(votes.shape, jnp.int32),
            pltpu.VMEM(elected.shape, jnp.int32),
            pltpu.SemaphoreType.DMA((len(cuts) + 7,)),
            pltpu.VMEM((leaves * padded, features), jnp.bfloat16),
        ],
        compiler_params=pltpu.CompilerParams(vmem_limit_bytes=48 << 20),
        name="local_stage",
    )(*[in_hbm(x) for x in (bins, leaf, score, level, rank, lengths, votes, elected)])


def gain_stage(packets, where, leaves, plan):
    devices = packets.shape[0]
    picks = plan["picks"]
    units = plan["units"]
    chunks = plan["chunks"]
    chunk = 4 if devices % 4 == 0 else 1
    even = units % HALVES == 0

    half = cdiv(chunks, 2)
    batch = 4

    def body(where_ref, packet_ref, out_ref, total_ref, grad_ref, hess_ref, late_ref):
        leaf_id = lax.broadcasted_iota(jnp.int32, (leaves, LANES), 0).astype(jnp.float32)
        bin_id = lax.broadcasted_iota(jnp.int32, (LANES, LANES), 0).astype(jnp.float32)
        local = []
        limit = []
        base = where_ref[0] % plan["owners"] * units
        first = jnp.minimum(base // HALVES, plan["padded"] - picks)
        for i in range(units):
            if even:
                local.append(i // HALVES)
                limit.append(bin_id + float(i % HALVES * LANES))
            else:
                local.append(jnp.clip((base + i) // HALVES - first, 0, picks - 1))
                limit.append(bin_id + ((base + i) % HALVES * LANES).astype(jnp.float32))
        def terms(tiles):
            weights = []
            steps = [[] for _ in range(units)]
            grad_sum = jnp.zeros((leaves, LANES), jnp.float32)
            hess_sum = jnp.zeros((leaves, LANES), jnp.float32)
            for s, c, valid in tiles:
                owner = packet_ref[s, c, picks : picks + 1, :]
                if valid is not None:
                    owner = jnp.where(valid, owner, -1.0)
                mine = owner == leaf_id
                grad = jnp.where(mine, packet_ref[s, c, picks + 1 : picks + 2, :], 0.0)
                hess = jnp.where(mine, packet_ref[s, c, picks + 2 : picks + 3, :], 0.0)
                grad_sum = grad_sum + grad
                hess_sum = hess_sum + hess
                grad_high = grad.astype(jnp.bfloat16)
                hess_high = hess.astype(jnp.bfloat16)
                grad_low = (grad - grad_high.astype(jnp.float32)).astype(jnp.bfloat16)
                hess_low = (hess - hess_high.astype(jnp.float32)).astype(jnp.bfloat16)
                weights.append(
                    jnp.concatenate([grad_high, hess_high, grad_low, hess_low], axis=0)
                )
                for i in range(units):
                    value = packet_ref[s, c, pl.ds(local[i], 1), :]
                    steps[i].append((value <= limit[i]).astype(jnp.float32).astype(jnp.bfloat16))
            weight = jnp.concatenate(weights, axis=1)
            step = jnp.concatenate([jnp.concatenate(p, axis=1) for p in steps], axis=0)
            product = lax.dot_general(
                weight, step, (((1,), (1,)), ((), ())), preferred_element_type=jnp.float32
            )
            return product, grad_sum, hess_sum

        late = jnp.int32(0)
        for c in range(half, chunks):
            for s0 in range(0, devices, 16):
                flag = jnp.zeros((1, LANES), jnp.float32)
                for s in range(s0, min(s0 + 16, devices)):
                    row = plan["vote_lines"]
                    count = packet_ref[s, chunks + row // plan["rows"], row % plan["rows"], :]
                    flag = flag + jnp.where(
                        count.reshape(1, LANES) > float(c * LANES), float(1 << (s - s0)), 0.0
                    )
                flag = jnp.max(flag).astype(jnp.int32)
                for s in range(s0, min(s0 + 16, devices)):
                    late_ref[late] = s * chunks + c
                    late = late + (jnp.right_shift(flag, s - s0) & 1)

        def listed(first):
            tiles = []
            for k in range(batch):
                valid = first + k < late
                tile = jnp.where(valid, late_ref[first + k], 0)
                tiles.append((tile // chunks, tile % chunks, valid))
            return tiles

        total = grad_all = hess_all = None
        for s0 in range(0, devices + 1, chunk):
            if s0 < devices:
                tiles = [(s, c, None) for s in range(s0, s0 + chunk) for c in range(half)]
            else:
                tiles = listed(0)
            more, grad_more, hess_more = terms(tiles)
            if s0:
                more = total + more
                grad_more = grad_all + grad_more
                hess_more = hess_all + hess_more
            total, grad_all, hess_all = more, grad_more, hess_more
        total_ref[...] = total
        grad_ref[...] = grad_all
        hess_ref[...] = hess_all

        def add(k, carry):
            more, grad_more, hess_more = terms(listed(k * batch))
            total_ref[...] += more
            grad_ref[...] += grad_more
            hess_ref[...] += hess_more
            return carry

        lax.fori_loop(1, jnp.maximum((late + batch - 1) // batch, 1), add, 0)
        total = total_ref[...]
        grad_all = grad_ref[...]
        hess_all = hess_ref[...]
        prefix_grad = total[0:leaves] + total[2 * leaves : 3 * leaves]
        prefix_hess = total[leaves : 2 * leaves] + total[3 * leaves :]
        whole_grad = jnp.sum(grad_all, axis=1, keepdims=True)
        whole_hess = jnp.sum(hess_all, axis=1, keepdims=True)
        rest_grad = whole_grad - prefix_grad
        rest_hess = whole_hess - prefix_hess
        gains = (
            prefix_grad * prefix_grad / (prefix_hess + ridge_weight)
            + rest_grad * rest_grad / (rest_hess + ridge_weight)
            - whole_grad * whole_grad / (whole_hess + ridge_weight)
        )
        for i in range(units):
            out_ref[i * leaves : (i + 1) * leaves, :] = gains[:, i * LANES : (i + 1) * LANES]

    vmem = pl.BlockSpec(memory_space=pltpu.VMEM)
    return pl.pallas_call(
        body,
        in_specs=[pl.BlockSpec(memory_space=pltpu.SMEM), vmem],
        out_specs=vmem,
        out_shape=vmem_array((units * leaves, LANES)),
        scratch_shapes=[
            pltpu.VMEM((4 * leaves, units * LANES), jnp.float32),
            pltpu.VMEM((leaves, LANES), jnp.float32),
            pltpu.VMEM((leaves, LANES), jnp.float32),
            pltpu.SMEM((devices * chunks + batch,), jnp.int32),
        ],
        compiler_params=pltpu.CompilerParams(vmem_limit_bytes=48 << 20),
        name="gain_stage",
    )(where, in_vmem(packets))


def vote_stage(packets, before, sources, features, leaves, kept, plan):
    rows = plan["rows"]
    lines = plan["vote_lines"]
    step = 64
    depth = round_up(features, LANES)
    last = before is not None

    def body(packet_ref, *refs):
        out_ref, count = refs[-2:] if last else (None, refs[-1])
        lane = lax.broadcasted_iota(jnp.int32, (1, LANES), 1)

        def block(index, carry):
            start = pl.multiple_of(index * step, step)
            feature = (lax.broadcasted_iota(jnp.int32, (step, LANES), 0) + start).astype(
                jnp.float32
            )
            total = jnp.zeros((step, LANES), jnp.float32)
            if last:
                total = refs[0][pl.ds(start, step), :]
            for s in sources:
                for line in range(lines):
                    row = line % rows
                    values = packet_ref[s, plan["chunks"] + line // rows, row : row + 1, :]
                    inside = kept * leaves - line * LANES
                    if inside < LANES:
                        values = jnp.where(lane < inside, values, -1.0)
                    total = total + (values == feature).astype(jnp.float32)
            count[pl.ds(start, step), :] = total
            return carry

        lax.fori_loop(0, depth // step, block, 0)
        if last:
            turned = count[...].T
            summed = turned[0:leaves]
            for i in range(1, LANES // leaves):
                summed = summed + turned[i * leaves : (i + 1) * leaves]
            out_ref[...] = summed[:, 0:features].astype(jnp.int32)

    vmem = pl.BlockSpec(memory_space=pltpu.VMEM)
    if last:
        inputs = [in_vmem(packets), in_vmem(before)]
        out_shape = jax.ShapeDtypeStruct((leaves, features), jnp.int32)
        scratch = [pltpu.VMEM((depth, LANES), jnp.float32)]
    else:
        inputs = [in_vmem(packets)]
        out_shape = vmem_array((depth, LANES))
        scratch = []
    return pl.pallas_call(
        body,
        in_specs=[vmem] * len(inputs),
        out_specs=vmem,
        out_shape=out_shape,
        scratch_shapes=scratch,
        compiler_params=pltpu.CompilerParams(vmem_limit_bytes=48 << 20),
        cost_estimate=pl.CostEstimate(flops=20_000_000, bytes_accessed=400_000, transcendentals=0),
        name="vote_stage",
    )(*inputs)


def place_stage(blocks, where, leaves, picked, plan):
    units = plan["units"]
    owners = plan["owners"]
    step = 8 if leaves % 8 == 0 else leaves

    rows = step * picked
    groups = leaves // step

    def body(where_ref, *refs):
        out_ref, planes, done = refs[-3:]
        here = where_ref[0] % owners
        odd = here & 1
        owner = []
        for index in range(len(blocks)):
            if not plan["doubling"]:
                owner.append(index)
                continue
            even_tag, odd_tag = plan["tags"][index % len(plan["tags"])]
            if index < len(plan["tags"]):
                owner.append(here ^ jnp.where(odd == 1, odd_tag, even_tag))
            else:
                owner.append(here ^ 1 ^ jnp.where(odd == 1, even_tag, odd_tag))
        copies = []
        for g in range(groups):
            for index, ref in enumerate(refs[:-3]):
                for i in range(units):

                    def write(index=index, ref=ref, i=i):
                        if units % HALVES == 0:
                            half = i % HALVES
                            pick = owner[index] * (units // HALVES) + i // HALVES
                        else:
                            half = (owner[index] * units + i) % HALVES
                            pick = (owner[index] * units + i) // HALVES
                        start = i * leaves + g * step
                        planes[half, pl.ds(g * rows + pick, step, stride=picked), :] = ref[
                            start : start + step, :
                        ]

                    if owners * units == picked * HALVES:
                        write()
                    else:
                        pl.when(owner[index] * units + i < picked * HALVES)(write)
            for half in range(HALVES):
                copy = pltpu.make_async_copy(
                    planes.at[half, pl.ds(g * rows, rows), :],
                    out_ref.at[pl.ds(g * rows, rows), pl.ds(half * LANES, LANES)],
                    done.at[g * HALVES + half],
                )
                copy.start()
                copies.append(copy)
        for copy in copies:
            copy.wait()

    vmem = pl.BlockSpec(memory_space=pltpu.VMEM)
    return pl.pallas_call(
        body,
        in_specs=[pl.BlockSpec(memory_space=pltpu.SMEM)] + [vmem] * len(blocks),
        out_specs=pl.BlockSpec(memory_space=pltpu.HBM),
        out_shape=jax.ShapeDtypeStruct((leaves * picked, B), jnp.float32),
        scratch_shapes=[
            pltpu.VMEM((HALVES, leaves * picked, LANES), jnp.float32),
            pltpu.SemaphoreType.DMA((groups * HALVES,)),
        ],
        compiler_params=pltpu.CompilerParams(vmem_limit_bytes=48 << 20),
        name="place_stage",
    )(where, *[in_vmem(b) for b in blocks]).reshape(leaves, picked, B)


def solution(mesh):
    devices = mesh.shape["rows"]

    def on_device(
        feature_bin, doc_leaf, current_score, relevance, doc_rank, query_length, feature_votes,
        elected,
    ):
        documents, features = feature_bin.shape
        leaves, picked = elected.shape
        kept = feature_votes.shape[2]
        doubling = devices >= 8 and devices & (devices - 1) == 0
        owners = devices // 2 if doubling else devices
        units = cdiv(picked * HALVES, owners)
        padded = round_up(picked, 8)
        picks = max(
            (j * units + units - 1) // HALVES - (j * units) // HALVES + 1 for j in range(owners)
        )
        rows = round_up(picks + 3, 8)
        plan = {
            "devices": devices,
            "doubling": doubling,
            "owners": owners,
            "units": units,
            "picks": picks,
            "padded": padded,
            "first": [min(j * units // HALVES, padded - picks) for j in range(owners)],
            "rows": rows,
            "chunks": documents // LANES,
            "vote_lines": cdiv(kept * leaves, LANES),
            "vote_tiles": cdiv(cdiv(kept * leaves, LANES) + 1, rows),
        }
        where = lax.axis_index("rows").astype(jnp.int32).reshape(1)
        gradient, hessian, packets = local_stage(
            feature_bin.T,
            doc_leaf.reshape(1, -1),
            current_score.reshape(1, -1),
            relevance.reshape(1, -1),
            doc_rank.reshape(1, -1),
            query_length,
            feature_votes.transpose(2, 0, 1),
            elected,
            plan,
        )
        received = lax.all_to_all(packets, "rows", 0, 0)
        block = gain_stage(received, where, leaves, plan)
        middle = cdiv(devices, 2)
        count_args = (features, leaves, kept, plan)
        votes = vote_stage(received, None, range(middle), *count_args)
        if doubling:
            far = [1 << b for b in reversed(range(1, owners.bit_length() - 1))]
            twin = list(far)
            twin[-2:] = twin[-2:][::-1]
            pairs = [
                [(i, i ^ (twin[p] if i & 1 else far[p])) for i in range(devices)]
                for p in range(len(far))
            ]
            tags = [(0, 0)]
            for p in range(len(far)):
                tags = tags + [(even | far[p], odd | twin[p]) for even, odd in tags]
            sibling = [(i, i ^ 1) for i in range(devices)]

            def send(b, pair):
                return lax.ppermute(b, "rows", pair)

            moved = send(block, pairs[0])
            again, votes = lax.optimization_barrier((block, votes))
            crossed = [send(again, sibling)]
            moved, votes = lax.optimization_barrier((moved, votes))
            blocks = [block, moved]
            for p in range(1, len(far)):
                moved = [send(b, pairs[p]) for b in [again] + blocks[1:]]
                if p == len(far) - 1:
                    votes = vote_stage(received, votes, range(middle, devices), *count_args)
                    waiting, votes = lax.optimization_barrier((blocks[1:] + moved[:-1], votes))
                    crossed = crossed + [send(b, sibling) for b in waiting]
                    moved[-1], votes = lax.optimization_barrier((moved[-1], votes))
                blocks = blocks + moved
            if len(far) == 1:
                votes = vote_stage(received, votes, range(middle, devices), *count_args)
            blocks = blocks + crossed + [send(blocks[-1], sibling)]
            plan["tags"] = tags
        else:
            votes = vote_stage(received, votes, range(middle, devices), *count_args)
            gathered = lax.all_gather(block, "rows", axis=0)
            blocks = [gathered[j] for j in range(devices)]
            plan["tags"] = None
        split_gain = place_stage(blocks, where, leaves, picked, plan)
        return gradient.reshape(-1), hessian.reshape(-1), votes, split_gain

    return jax.shard_map(
        on_device,
        mesh=mesh,
        in_specs=(
            P(("parts", "rows"), None),
            P(("parts", "rows")),
            P(("parts", "rows")),
            P(("parts", "rows")),
            P(("parts", "rows")),
            P(("parts", "rows")),
            P(("parts", "rows"), None, None),
            P("parts", None),
        ),
        out_specs=(
            P(("parts", "rows")),
            P(("parts", "rows")),
            P("parts", None),
            P("parts", None, None),
        ),
        check_vma=False,
    )
```

```python
import jax
import jax.numpy as jnp
from jax import lax
from jax.experimental import pallas as pl
from jax.experimental.pallas import tpu as pltpu
from jax.sharding import PartitionSpec as P


B = 256
LANES = 128
HALVES = B // LANES
LEVELS = 4

ridge_weight = 1.0


def cdiv(a, b):
    return -(-a // b)


def round_up(a, b):
    return cdiv(a, b) * b


def query_rows(score, level, rank, lengths, slots):
    documents = score.shape[1]
    queries = documents // slots
    gain = jnp.left_shift(1, level).astype(jnp.float32) - 1.0
    discount = 1.0 / jnp.log2(rank.astype(jnp.float32) + 2.0)
    place = lax.broadcasted_iota(jnp.int32, (1, slots), 1)
    place_discount = 1.0 / jnp.log2(place.astype(jnp.float32) + 2.0)
    gradients = []
    hessians = []
    for q in range(queries):
        lanes = slice(q * slots, (q + 1) * slots)
        live = place < lengths[q]
        live_row = live.astype(jnp.float32)
        score_row = score[:, lanes]
        gain_row = gain[:, lanes]
        discount_row = discount[:, lanes]
        level_row = jnp.where(live, level[:, lanes], -1)
        ideal_gain = jnp.zeros((1, slots), jnp.float32)
        for v in range(1, LEVELS + 1):
            count = jnp.sum((level_row >= v).astype(jnp.float32), axis=1, keepdims=True)
            ideal_gain = ideal_gain + jnp.where(
                place.astype(jnp.float32) < count, float(2 ** (v - 1)), 0.0
            )
        ideal = jnp.sum(ideal_gain * place_discount, axis=1, keepdims=True)
        scaling = 1.0 / jnp.maximum(ideal, 1.0)
        rows = jnp.concatenate(
            [score_row, gain_row, discount_row, live_row, jnp.zeros((4, slots), jnp.float32)],
            axis=0,
        )
        columns = rows.T
        step = 32
        push_sum = jnp.zeros((8, slots), jnp.float32)
        curve_sum = jnp.zeros((8, slots), jnp.float32)
        for r in range(0, slots, step):
            part = columns[r : r + step]
            gap = (part[:, 1:2] - gain_row) * part[:, 3:4]
            change = gap * jnp.abs(part[:, 2:3] - discount_row)
            lead = score_row - part[:, 0:1]
            chance = 1.0 / (1.0 + jnp.exp(jnp.where(gap > 0.0, -lead, lead)))
            push = chance * change
            curve = (1.0 - chance) * jnp.abs(push)
            for k in range(0, step, 8):
                push_sum = push_sum + push[k : k + 8]
                curve_sum = curve_sum + curve[k : k + 8]
        factor = scaling * live_row
        gradients.append(jnp.sum(push_sum, axis=0, keepdims=True) * factor)
        hessians.append(jnp.sum(curve_sum, axis=0, keepdims=True) * factor)
    return jnp.concatenate(gradients, axis=1), jnp.concatenate(hessians, axis=1)


def vmem_array(shape):
    return pltpu.VMEM(shape, jnp.float32)


def in_vmem(x):
    return pltpu.with_memory_space_constraint(x, pltpu.VMEM)


def in_hbm(x):
    return pltpu.with_memory_space_constraint(x, pltpu.HBM)


def local_stage(bins, leaf, score, level, rank, lengths, votes, elected, plan):
    features, documents = bins.shape
    leaves, picked = elected.shape
    kept = votes.shape[0]
    padded = plan["padded"]
    picks = plan["picks"]
    rows = plan["rows"]
    slots = documents // lengths.shape[0]
    group = 8 if leaves % 8 == 0 else leaves
    per_row = LANES // leaves

    piece = round_up(cdiv(features, 4), 8)
    cuts = [(f, min(piece, features - f)) for f in range(0, features, piece)]

    def body(*refs):
        sources = refs[0:8]
        grad_ref, hess_ref, packet_ref = refs[8:11]
        square, chosen_ref = refs[11:13]
        copied = refs[13:21]
        arrived = refs[21]
        bins_here, leaf_ref, score_ref, level_ref, rank_ref, length_ref, votes_ref, elected_ref = (
            copied
        )
        small = [
            pltpu.make_async_copy(sources[k], copied[k], arrived.at[len(cuts) + k - 1])
            for k in (5, 2, 3, 4, 7, 1, 6)
        ]
        fetches = [
            pltpu.make_async_copy(
                sources[0].at[pl.ds(f, size), :], bins_here.at[pl.ds(f, size), :], arrived.at[k]
            )
            for k, (f, size) in enumerate(cuts)
        ]
        for copy in small + fetches:
            copy.start()
        for copy in small:
            copy.wait()
        square[...] = jnp.zeros(square.shape, jnp.float32)
        square[0:leaves, 0:picked] = elected_ref[...].astype(jnp.float32)
        elected_t = square[...].T
        leaf_row = leaf_ref[...]
        gradient, hessian = query_rows(
            score_ref[...], level_ref[...], rank_ref[...], length_ref, slots
        )
        grad_ref[...] = gradient
        hess_ref[...] = hessian
        lane = lax.broadcasted_iota(jnp.int32, (1, documents), 1)
        starts = [0]
        for q in range(documents // slots):
            starts.append(starts[-1] + length_ref[q])

        def compact(block):
            result = block
            for q in range(1, documents // slots):
                moved = pltpu.roll(block, starts[q] - q * slots + documents, 1)
                result = jnp.where(lane >= starts[q], moved, result)
            return result

        shared = [leaf_row.astype(jnp.float32), gradient, hessian]
        shared.append(jnp.zeros((max(rows - picks, 8) - 3, documents), jnp.float32))
        shared = compact(jnp.concatenate(shared, axis=0))[0 : rows - picks]
        shared = jnp.where(lane < starts[-1], shared, 0.0)
        count = jnp.zeros((1, LANES), jnp.float32) + starts[-1].astype(jnp.float32)
        feature = lax.broadcasted_iota(jnp.int32, (padded, features), 1).astype(jnp.float32)
        for fetch in fetches:
            fetch.wait()
        table = bins_here[...].astype(jnp.float32).astype(jnp.bfloat16)
        chosen = jnp.zeros((padded, documents), jnp.float32)
        for first in range(0, leaves, group):
            hot = []
            for l in range(first, first + group):
                hot.append((elected_t[0:padded, l : l + 1] == feature).astype(jnp.float32))
            hot = jnp.concatenate(hot, axis=0).astype(jnp.bfloat16)
            found = jnp.dot(hot, table, preferred_element_type=jnp.float32)
            for i in range(group):
                chosen = jnp.where(
                    leaf_row == first + i, found[i * padded : (i + 1) * padded], chosen
                )
        chosen_ref[...] = compact(chosen)
        tail = []
        for k0 in range(0, kept, per_row):
            line = jnp.zeros((1, LANES), jnp.float32)
            for i in range(min(per_row, kept - k0)):
                values = votes_ref[k0 + i].astype(jnp.float32)
                pieces = [values]
                if i:
                    pieces.insert(0, jnp.zeros((1, i * leaves), jnp.float32))
                if (i + 1) * leaves < LANES:
                    pieces.append(jnp.zeros((1, LANES - (i + 1) * leaves), jnp.float32))
                line = line + jnp.concatenate(pieces, axis=1)
            tail.append(line)
        tail.append(count)
        spare = plan["vote_tiles"] * rows - len(tail)
        if spare:
            tail.append(jnp.zeros((spare, LANES), jnp.float32))
        tail = jnp.concatenate(tail, axis=0)
        for j in range(plan["devices"]):
            start = plan["first"][j % plan["owners"]]
            block = jnp.concatenate([chosen_ref[start : start + picks, :], shared], axis=0)
            for c in range(documents // LANES):
                packet_ref[j, c] = block[:, c * LANES : (c + 1) * LANES]
            for t in range(plan["vote_tiles"]):
                packet_ref[j, documents // LANES + t] = tail[t * rows : (t + 1) * rows]

    vmem = pl.BlockSpec(memory_space=pltpu.VMEM)
    return pl.pallas_call(
        body,
        in_specs=[pl.BlockSpec(memory_space=pltpu.HBM)] * 8,
        out_specs=[vmem] * 3,
        out_shape=[
            jax.ShapeDtypeStruct((1, documents), jnp.float32),
            jax.ShapeDtypeStruct((1, documents), jnp.float32),
            vmem_array(
                (plan["devices"], documents // LANES + plan["vote_tiles"], rows, LANES)
            ),
        ],
        scratch_shapes=[
            pltpu.VMEM((LANES, LANES), jnp.float32),
            pltpu.VMEM((padded, documents), jnp.float32),
            pltpu.VMEM((features, documents), jnp.int32),
            pltpu.VMEM((1, documents), jnp.int32),
            pltpu.VMEM((1, documents), jnp.float32),
            pltpu.VMEM((1, documents), jnp.int32),
            pltpu.VMEM((1, documents), jnp.int32),
            pltpu.SMEM(lengths.shape, jnp.int32),
            pltpu.VMEM(votes.shape, jnp.int32),
            pltpu.VMEM(elected.shape, jnp.int32),
            pltpu.SemaphoreType.DMA((len(cuts) + 7,)),
        ],
        compiler_params=pltpu.CompilerParams(vmem_limit_bytes=48 << 20),
        name="local_stage",
    )(*[in_hbm(x) for x in (bins, leaf, score, level, rank, lengths, votes, elected)])


def gain_stage(packets, where, leaves, low, high, earlier, plan):
    devices = packets.shape[0]
    picks = plan["picks"]
    units = high - low
    chunks = plan["chunks"]
    chunk = 4 if devices % 4 == 0 else 1
    even = plan["units"] % HALVES == 0

    half = cdiv(chunks, 2)
    batch = 4

    def body(where_ref, packet_ref, *refs):
        total_ref, grad_ref, hess_ref, late_ref = refs[-4:]
        out_ref = refs[len(before)]
        leaf_id = lax.broadcasted_iota(jnp.int32, (leaves, LANES), 0).astype(jnp.float32)
        bin_id = lax.broadcasted_iota(jnp.int32, (LANES, LANES), 0).astype(jnp.float32)
        local = []
        limit = []
        base = where_ref[0] % plan["owners"] * plan["units"]
        first = jnp.minimum(base // HALVES, plan["padded"] - picks)
        for i in range(low, high):
            if even:
                local.append(i // HALVES)
                limit.append(bin_id + float(i % HALVES * LANES))
            else:
                local.append(jnp.clip((base + i) // HALVES - first, 0, picks - 1))
                limit.append(bin_id + ((base + i) % HALVES * LANES).astype(jnp.float32))

        def terms(tiles):
            weights = []
            steps = [[] for _ in range(units)]
            grad_sum = jnp.zeros((leaves, LANES), jnp.float32)
            hess_sum = jnp.zeros((leaves, LANES), jnp.float32)
            for s, c, valid in tiles:
                owner = packet_ref[s, c, picks : picks + 1, :]
                if valid is not None:
                    owner = jnp.where(valid, owner, -1.0)
                mine = owner == leaf_id
                grad = jnp.where(mine, packet_ref[s, c, picks + 1 : picks + 2, :], 0.0)
                hess = jnp.where(mine, packet_ref[s, c, picks + 2 : picks + 3, :], 0.0)
                grad_sum = grad_sum + grad
                hess_sum = hess_sum + hess
                grad_high = grad.astype(jnp.bfloat16)
                hess_high = hess.astype(jnp.bfloat16)
                grad_low = (grad - grad_high.astype(jnp.float32)).astype(jnp.bfloat16)
                hess_low = (hess - hess_high.astype(jnp.float32)).astype(jnp.bfloat16)
                weights.append(
                    jnp.concatenate([grad_high, hess_high, grad_low, hess_low], axis=0)
                )
                for i in range(units):
                    value = packet_ref[s, c, pl.ds(local[i], 1), :]
                    steps[i].append((value <= limit[i]).astype(jnp.float32).astype(jnp.bfloat16))
            weight = jnp.concatenate(weights, axis=1)
            step = jnp.concatenate([jnp.concatenate(p, axis=1) for p in steps], axis=0)
            product = lax.dot_general(
                weight, step, (((1,), (1,)), ((), ())), preferred_element_type=jnp.float32
            )
            return product, grad_sum, hess_sum

        late = jnp.int32(0)
        for c in range(half, chunks):
            for s0 in range(0, devices, 16):
                flag = jnp.zeros((1, LANES), jnp.float32)
                for s in range(s0, min(s0 + 16, devices)):
                    row = plan["vote_lines"]
                    count = packet_ref[s, chunks + row // plan["rows"], row % plan["rows"], :]
                    flag = flag + jnp.where(
                        count.reshape(1, LANES) > float(c * LANES), float(1 << (s - s0)), 0.0
                    )
                flag = jnp.max(flag).astype(jnp.int32)
                for s in range(s0, min(s0 + 16, devices)):
                    late_ref[late] = s * chunks + c
                    late = late + (jnp.right_shift(flag, s - s0) & 1)

        def listed(first):
            tiles = []
            for k in range(batch):
                valid = first + k < late
                tile = jnp.where(valid, late_ref[first + k], 0)
                tiles.append((tile // chunks, tile % chunks, valid))
            return tiles

        total = grad_all = hess_all = None
        for s0 in range(0, devices + 1, chunk):
            if s0 < devices:
                tiles = [(s, c, None) for s in range(s0, s0 + chunk) for c in range(half)]
            else:
                tiles = listed(0)
            more, grad_more, hess_more = terms(tiles)
            if s0:
                more = total + more
                grad_more = grad_all + grad_more
                hess_more = hess_all + hess_more
            total, grad_all, hess_all = more, grad_more, hess_more
        total_ref[...] = total
        grad_ref[...] = grad_all
        hess_ref[...] = hess_all

        def add(k, carry):
            more, grad_more, hess_more = terms(listed(k * batch))
            total_ref[...] += more
            grad_ref[...] += grad_more
            hess_ref[...] += hess_more
            return carry

        lax.fori_loop(1, jnp.maximum((late + batch - 1) // batch, 1), add, 0)
        total = total_ref[...]
        grad_all = grad_ref[...]
        hess_all = hess_ref[...]
        prefix_grad = total[0:leaves] + total[2 * leaves : 3 * leaves]
        prefix_hess = total[leaves : 2 * leaves] + total[3 * leaves :]
        whole_grad = jnp.sum(grad_all, axis=1, keepdims=True)
        whole_hess = jnp.sum(hess_all, axis=1, keepdims=True)
        rest_grad = whole_grad - prefix_grad
        rest_hess = whole_hess - prefix_hess
        gains = (
            prefix_grad * prefix_grad / (prefix_hess + ridge_weight)
            + rest_grad * rest_grad / (rest_hess + ridge_weight)
            - whole_grad * whole_grad / (whole_hess + ridge_weight)
        )
        for i in range(units):
            out_ref[i * leaves : (i + 1) * leaves, :] = gains[:, i * LANES : (i + 1) * LANES]
        if before:
            whole_ref = refs[len(before) + 1]
            whole_ref[0 : low * leaves, :] = refs[0][...]
            whole_ref[low * leaves :, :] = out_ref[...]

    before = [] if earlier is None else [in_vmem(earlier)]
    shapes = [vmem_array((units * leaves, LANES))]
    if before:
        shapes.append(vmem_array((high * leaves, LANES)))
    vmem = pl.BlockSpec(memory_space=pltpu.VMEM)
    return pl.pallas_call(
        body,
        in_specs=[pl.BlockSpec(memory_space=pltpu.SMEM), vmem] + [vmem] * len(before),
        out_specs=[vmem] * len(shapes),
        out_shape=shapes,
        scratch_shapes=[
            pltpu.VMEM((4 * leaves, units * LANES), jnp.float32),
            pltpu.VMEM((leaves, LANES), jnp.float32),
            pltpu.VMEM((leaves, LANES), jnp.float32),
            pltpu.SMEM((devices * chunks + batch,), jnp.int32),
        ],
        compiler_params=pltpu.CompilerParams(vmem_limit_bytes=48 << 20),
        name="gain_stage",
    )(where, in_vmem(packets), *before)


def vote_stage(packets, before, sources, last, features, leaves, kept, plan):
    rows = plan["rows"]
    lines = plan["vote_lines"]
    step = 64
    depth = round_up(features, LANES)
    inputs = [in_vmem(packets)] + ([] if before is None else [in_vmem(before)])

    def body(packet_ref, *refs):
        out_ref, count = refs[-2:] if last else (None, refs[-1])
        lane = lax.broadcasted_iota(jnp.int32, (1, LANES), 1)

        def block(index, carry):
            start = pl.multiple_of(index * step, step)
            feature = (lax.broadcasted_iota(jnp.int32, (step, LANES), 0) + start).astype(
                jnp.float32
            )
            total = jnp.zeros((step, LANES), jnp.float32)
            if before is not None:
                total = refs[0][pl.ds(start, step), :]
            for s in sources:
                for line in range(lines):
                    row = line % rows
                    values = packet_ref[s, plan["chunks"] + line // rows, row : row + 1, :]
                    inside = kept * leaves - line * LANES
                    if inside < LANES:
                        values = jnp.where(lane < inside, values, -1.0)
                    total = total + (values == feature).astype(jnp.float32)
            count[pl.ds(start, step), :] = total
            return carry

        lax.fori_loop(0, depth // step, block, 0)
        if last:
            turned = count[...].T
            summed = turned[0:leaves]
            for i in range(1, LANES // leaves):
                summed = summed + turned[i * leaves : (i + 1) * leaves]
            out_ref[...] = summed[:, 0:features].astype(jnp.int32)

    vmem = pl.BlockSpec(memory_space=pltpu.VMEM)
    if last:
        out_shape = jax.ShapeDtypeStruct((leaves, features), jnp.int32)
        scratch = [pltpu.VMEM((depth, LANES), jnp.float32)]
    else:
        out_shape = vmem_array((depth, LANES))
        scratch = []
    return pl.pallas_call(
        body,
        in_specs=[vmem] * len(inputs),
        out_specs=vmem,
        out_shape=out_shape,
        scratch_shapes=scratch,
        compiler_params=pltpu.CompilerParams(vmem_limit_bytes=48 << 20),
        cost_estimate=pl.CostEstimate(flops=20_000_000, bytes_accessed=400_000, transcendentals=0),
        name="vote_stage",
    )(*inputs)


def place_stage(blocks, tags, spans, where, leaves, picked, plan):
    units = plan["units"]
    owners = plan["owners"]
    step = 8 if leaves % 8 == 0 else leaves

    rows = step * picked
    groups = leaves // step

    def body(where_ref, *refs):
        out_ref, planes, done = refs[-3:]
        here = where_ref[0] % owners
        odd = here & 1
        owner = []
        for index in range(len(blocks)):
            if not plan["doubling"]:
                owner.append(index)
                continue
            even_tag, odd_tag = tags[index][0:2]
            if not tags[index][2]:
                owner.append(here ^ jnp.where(odd == 1, odd_tag, even_tag))
            else:
                owner.append(here ^ 1 ^ jnp.where(odd == 1, even_tag, odd_tag))
        copies = []
        for g in range(groups):
            for index, ref in enumerate(refs[:-3]):
                low, high = spans[index]
                for i in range(low, high):

                    def write(index=index, ref=ref, i=i, low=low):
                        if units % HALVES == 0:
                            half = i % HALVES
                            pick = owner[index] * (units // HALVES) + i // HALVES
                        else:
                            half = (owner[index] * units + i) % HALVES
                            pick = (owner[index] * units + i) // HALVES
                        start = (i - low) * leaves + g * step
                        planes[half, pl.ds(g * rows + pick, step, stride=picked), :] = ref[
                            start : start + step, :
                        ]

                    if owners * units == picked * HALVES:
                        write()
                    else:
                        pl.when(owner[index] * units + i < picked * HALVES)(write)
            for half in range(HALVES):
                copy = pltpu.make_async_copy(
                    planes.at[half, pl.ds(g * rows, rows), :],
                    out_ref.at[pl.ds(g * rows, rows), pl.ds(half * LANES, LANES)],
                    done.at[g * HALVES + half],
                )
                copy.start()
                copies.append(copy)
        for copy in copies:
            copy.wait()

    vmem = pl.BlockSpec(memory_space=pltpu.VMEM)
    return pl.pallas_call(
        body,
        in_specs=[pl.BlockSpec(memory_space=pltpu.SMEM)] + [vmem] * len(blocks),
        out_specs=pl.BlockSpec(memory_space=pltpu.HBM),
        out_shape=jax.ShapeDtypeStruct((leaves * picked, B), jnp.float32),
        scratch_shapes=[
            pltpu.VMEM((HALVES, leaves * picked, LANES), jnp.float32),
            pltpu.SemaphoreType.DMA((groups * HALVES,)),
        ],
        compiler_params=pltpu.CompilerParams(vmem_limit_bytes=48 << 20),
        name="place_stage",
    )(where, *[in_vmem(b) for b in blocks]).reshape(leaves, picked, B)


def solution(mesh):
    devices = mesh.shape["rows"]

    def on_device(
        feature_bin, doc_leaf, current_score, relevance, doc_rank, query_length, feature_votes,
        elected,
    ):
        documents, features = feature_bin.shape
        leaves, picked = elected.shape
        kept = feature_votes.shape[2]
        doubling = devices >= 8 and devices & (devices - 1) == 0
        owners = devices // 2 if doubling else devices
        units = max(cdiv(picked * HALVES, owners), 2)
        padded = round_up(picked, 8)
        picks = max(
            (j * units + units - 1) // HALVES - (j * units) // HALVES + 1 for j in range(owners)
        )
        rows = round_up(picks + 3, 8)
        plan = {
            "devices": devices,
            "doubling": doubling,
            "owners": owners,
            "units": units,
            "picks": picks,
            "padded": padded,
            "first": [min(j * units // HALVES, padded - picks) for j in range(owners)],
            "rows": rows,
            "chunks": documents // LANES,
            "vote_lines": cdiv(kept * leaves, LANES),
            "vote_tiles": cdiv(cdiv(kept * leaves, LANES) + 1, rows),
        }
        where = lax.axis_index("rows").astype(jnp.int32).reshape(1)
        gradient, hessian, packets = local_stage(
            feature_bin.T,
            doc_leaf.reshape(1, -1),
            current_score.reshape(1, -1),
            relevance.reshape(1, -1),
            doc_rank.reshape(1, -1),
            query_length,
            feature_votes.transpose(2, 0, 1),
            elected,
            plan,
        )
        received = lax.all_to_all(packets, "rows", 0, 0)
        counters = (features, leaves, kept, plan)
        third = cdiv(devices, 3)
        shares = [range(min(k * third, devices), min((k + 1) * third, devices)) for k in range(3)]
        cut = units * 3 // 5
        if units % HALVES == 0:
            cut = max(cut // HALVES, 1) * HALVES if units > HALVES else 1
        (part,) = gain_stage(received, where, leaves, 0, cut, None, plan)
        rest, block = gain_stage(received, where, leaves, cut, units, part, plan)
        votes = vote_stage(received, None, shares[0], False, *counters)
        if doubling:
            far = [1 << b for b in reversed(range(1, owners.bit_length() - 1))]
            twin = list(far)
            twin[-2:] = twin[-2:][::-1]
            pairs = [
                [(i, i ^ (twin[p] if i & 1 else far[p])) for i in range(devices)]
                for p in range(len(far))
            ]
            sibling = [(i, i ^ 1) for i in range(devices)]

            def send(items, p):
                return [
                    (lax.ppermute(b, "rows", pairs[p]), even ^ far[p], odd ^ twin[p], low, high)
                    for b, even, odd, low, high in items
                ]

            def cross(items):
                return [(lax.ppermute(item[0], "rows", sibling),) + item[1:] for item in items]

            def after(items, other):
                arrays, other = lax.optimization_barrier(([item[0] for item in items], other))
                return [(b,) + item[1:] for b, item in zip(arrays, items)], other

            own = [(block, 0, 0, 0, units)]
            first = send([(part, 0, 0, 0, cut)], 0)
            second = send([(rest, 0, 0, cut, units)], 0)
            crossed = cross(own)
            first, votes = after(first, votes)
            votes = vote_stage(received, votes, shares[1], False, *counters)
            second, votes = after(second, votes)
            votes = vote_stage(received, votes, shares[2], True, *counters)
            items = own + first + second
            for p in range(1, len(far)):
                if p < len(far) - 1:
                    items = items + send(items, p)
                    continue
                moved = send(own, p)
                moved = moved + send(items[1:-1], p)
                moved = moved + send(items[-1:], p)
                crossed = crossed + cross(items[1:] + moved[:-2])
                crossed = crossed + cross(moved[-2:-1])
                crossed[-3:], joint = after(crossed[-3:], (moved[-1][0], votes))
                moved[-1] = (joint[0],) + moved[-1][1:]
                votes = joint[1]
                crossed = crossed + cross(moved[-1:])
                items = items + moved
            if len(far) == 1:
                crossed = crossed + cross(items[1:])
            tags = [item[1:3] + (False,) for item in items]
            tags = tags + [item[1:3] + (True,) for item in crossed]
            spans = [item[3:5] for item in items + crossed]
            blocks = [item[0] for item in items + crossed]
        else:
            votes = vote_stage(received, votes, range(third, devices), True, *counters)
            gathered = lax.all_gather(block, "rows", axis=0)
            blocks = [gathered[j] for j in range(devices)]
            tags = None
            spans = [(0, units)] * devices
        split_gain = place_stage(blocks, tags, spans, where, leaves, picked, plan)
        return gradient.reshape(-1), hessian.reshape(-1), votes, split_gain


    return jax.shard_map(
        on_device,
        mesh=mesh,
        in_specs=(
            P(("parts", "rows"), None),
            P(("parts", "rows")),
            P(("parts", "rows")),
            P(("parts", "rows")),
            P(("parts", "rows")),
            P(("parts", "rows")),
            P(("parts", "rows"), None, None),
            P("parts", None),
        ),
        out_specs=(
            P(("parts", "rows")),
            P(("parts", "rows")),
            P("parts", None),
            P("parts", None, None),
        ),
        check_vma=False,
    )
```

```python
import jax
import jax.numpy as jnp
from jax import lax
from jax.experimental import pallas as pl
from jax.experimental.pallas import tpu as pltpu
from jax.sharding import PartitionSpec as P


B = 256
LANES = 128
HALVES = B // LANES
LEVELS = 4

ridge_weight = 1.0


def cdiv(a, b):
    return -(-a // b)


def round_up(a, b):
    return cdiv(a, b) * b


def query_rows(score, level, rank, lengths, slots):
    documents = score.shape[1]
    queries = documents // slots
    gain = jnp.left_shift(1, level).astype(jnp.float32) - 1.0
    discount = 1.0 / jnp.log2(rank.astype(jnp.float32) + 2.0)
    place = lax.broadcasted_iota(jnp.int32, (1, slots), 1)
    place_discount = 1.0 / jnp.log2(place.astype(jnp.float32) + 2.0)
    gradients = []
    hessians = []
    for q in range(queries):
        lanes = slice(q * slots, (q + 1) * slots)
        live = place < lengths[q]
        live_row = live.astype(jnp.float32)
        score_row = score[:, lanes]
        gain_row = gain[:, lanes]
        discount_row = discount[:, lanes]
        level_row = jnp.where(live, level[:, lanes], -1)
        ideal_gain = jnp.zeros((1, slots), jnp.float32)
        for v in range(1, LEVELS + 1):
            count = jnp.sum((level_row >= v).astype(jnp.float32), axis=1, keepdims=True)
            ideal_gain = ideal_gain + jnp.where(
                place.astype(jnp.float32) < count, float(2 ** (v - 1)), 0.0
            )
        ideal = jnp.sum(ideal_gain * place_discount, axis=1, keepdims=True)
        scaling = 1.0 / jnp.maximum(ideal, 1.0)
        rows = jnp.concatenate(
            [score_row, gain_row, discount_row, live_row, jnp.zeros((4, slots), jnp.float32)],
            axis=0,
        )
        columns = rows.T
        step = 32
        push_sum = jnp.zeros((8, slots), jnp.float32)
        curve_sum = jnp.zeros((8, slots), jnp.float32)
        for r in range(0, slots, step):
            part = columns[r : r + step]
            gap = (part[:, 1:2] - gain_row) * part[:, 3:4]
            change = gap * jnp.abs(part[:, 2:3] - discount_row)
            lead = score_row - part[:, 0:1]
            chance = 1.0 / (1.0 + jnp.exp(jnp.where(gap > 0.0, -lead, lead)))
            push = chance * change
            curve = (1.0 - chance) * jnp.abs(push)
            for k in range(0, step, 8):
                push_sum = push_sum + push[k : k + 8]
                curve_sum = curve_sum + curve[k : k + 8]
        factor = scaling * live_row
        gradients.append(jnp.sum(push_sum, axis=0, keepdims=True) * factor)
        hessians.append(jnp.sum(curve_sum, axis=0, keepdims=True) * factor)
    return jnp.concatenate(gradients, axis=1), jnp.concatenate(hessians, axis=1)


def vmem_array(shape):
    return pltpu.VMEM(shape, jnp.float32)


def in_vmem(x):
    return pltpu.with_memory_space_constraint(x, pltpu.VMEM)


def in_hbm(x):
    return pltpu.with_memory_space_constraint(x, pltpu.HBM)


def local_stage(bins, leaf, score, level, rank, lengths, votes, elected, plan):
    features, documents = bins.shape
    leaves, picked = elected.shape
    kept = votes.shape[0]
    padded = plan["padded"]
    picks = plan["picks"]
    rows = plan["rows"]
    slots = documents // lengths.shape[0]
    group = 8 if leaves % 8 == 0 else leaves
    per_row = LANES // leaves

    piece = round_up(cdiv(features, 4), 8)
    cuts = [(f, min(piece, features - f)) for f in range(0, features, piece)]

    def body(*refs):
        sources = refs[0:8]
        grad_ref, hess_ref, packet_ref = refs[8:11]
        square, chosen_ref = refs[11:13]
        copied = refs[13:21]
        arrived = refs[21]
        bins_here, leaf_ref, score_ref, level_ref, rank_ref, length_ref, votes_ref, elected_ref = (
            copied
        )
        small = [
            pltpu.make_async_copy(sources[k], copied[k], arrived.at[len(cuts) + k - 1])
            for k in (5, 2, 3, 4, 7, 1, 6)
        ]
        fetches = [
            pltpu.make_async_copy(
                sources[0].at[pl.ds(f, size), :], bins_here.at[pl.ds(f, size), :], arrived.at[k]
            )
            for k, (f, size) in enumerate(cuts)
        ]
        for copy in small + fetches:
            copy.start()
        for copy in small:
            copy.wait()
        square[...] = jnp.zeros(square.shape, jnp.float32)
        square[0:leaves, 0:picked] = elected_ref[...].astype(jnp.float32)
        elected_t = square[...].T
        leaf_row = leaf_ref[...]
        gradient, hessian = query_rows(
            score_ref[...], level_ref[...], rank_ref[...], length_ref, slots
        )
        grad_ref[...] = gradient
        hess_ref[...] = hessian
        lane = lax.broadcasted_iota(jnp.int32, (1, documents), 1)
        starts = [0]
        for q in range(documents // slots):
            starts.append(starts[-1] + length_ref[q])

        def compact(block):
            result = block
            for q in range(1, documents // slots):
                moved = pltpu.roll(block, starts[q] - q * slots + documents, 1)
                result = jnp.where(lane >= starts[q], moved, result)
            return result

        shared = [leaf_row.astype(jnp.float32), gradient, hessian]
        shared.append(jnp.zeros((max(rows - picks, 8) - 3, documents), jnp.float32))
        shared = compact(jnp.concatenate(shared, axis=0))[0 : rows - picks]
        shared = jnp.where(lane < starts[-1], shared, 0.0)
        count = jnp.zeros((1, LANES), jnp.float32) + starts[-1].astype(jnp.float32)
        feature = lax.broadcasted_iota(jnp.int32, (padded, features), 1).astype(jnp.float32)
        for fetch in fetches:
            fetch.wait()
        table = bins_here[...].astype(jnp.float32).astype(jnp.bfloat16)
        chosen = jnp.zeros((padded, documents), jnp.float32)
        for first in range(0, leaves, group):
            hot = []
            for l in range(first, first + group):
                hot.append((elected_t[0:padded, l : l + 1] == feature).astype(jnp.float32))
            hot = jnp.concatenate(hot, axis=0).astype(jnp.bfloat16)
            found = jnp.dot(hot, table, preferred_element_type=jnp.float32)
            for i in range(group):
                chosen = jnp.where(
                    leaf_row == first + i, found[i * padded : (i + 1) * padded], chosen
                )
        chosen_ref[...] = compact(chosen)
        tail = []
        for k0 in range(0, kept, per_row):
            line = jnp.zeros((1, LANES), jnp.float32)
            for i in range(min(per_row, kept - k0)):
                values = votes_ref[k0 + i].astype(jnp.float32)
                pieces = [values]
                if i:
                    pieces.insert(0, jnp.zeros((1, i * leaves), jnp.float32))
                if (i + 1) * leaves < LANES:
                    pieces.append(jnp.zeros((1, LANES - (i + 1) * leaves), jnp.float32))
                line = line + jnp.concatenate(pieces, axis=1)
            tail.append(line)
        tail.append(count)
        spare = plan["vote_tiles"] * rows - len(tail)
        if spare:
            tail.append(jnp.zeros((spare, LANES), jnp.float32))
        tail = jnp.concatenate(tail, axis=0)
        for j in range(plan["devices"]):
            start = plan["first"][j % plan["owners"]]
            block = jnp.concatenate([chosen_ref[start : start + picks, :], shared], axis=0)
            for c in range(documents // LANES):
                packet_ref[j, c] = block[:, c * LANES : (c + 1) * LANES]
            for t in range(plan["vote_tiles"]):
                packet_ref[j, documents // LANES + t] = tail[t * rows : (t + 1) * rows]

    vmem = pl.BlockSpec(memory_space=pltpu.VMEM)
    return pl.pallas_call(
        body,
        in_specs=[pl.BlockSpec(memory_space=pltpu.HBM)] * 8,
        out_specs=[vmem] * 3,
        out_shape=[
            jax.ShapeDtypeStruct((1, documents), jnp.float32),
            jax.ShapeDtypeStruct((1, documents), jnp.float32),
            vmem_array(
                (plan["devices"], documents // LANES + plan["vote_tiles"], rows, LANES)
            ),
        ],
        scratch_shapes=[
            pltpu.VMEM((LANES, LANES), jnp.float32),
            pltpu.VMEM((padded, documents), jnp.float32),
            pltpu.VMEM((features, documents), jnp.int32),
            pltpu.VMEM((1, documents), jnp.int32),
            pltpu.VMEM((1, documents), jnp.float32),
            pltpu.VMEM((1, documents), jnp.int32),
            pltpu.VMEM((1, documents), jnp.int32),
            pltpu.SMEM(lengths.shape, jnp.int32),
            pltpu.VMEM(votes.shape, jnp.int32),
            pltpu.VMEM(elected.shape, jnp.int32),
            pltpu.SemaphoreType.DMA((len(cuts) + 7,)),
        ],
        compiler_params=pltpu.CompilerParams(vmem_limit_bytes=48 << 20),
        name="local_stage",
    )(*[in_hbm(x) for x in (bins, leaf, score, level, rank, lengths, votes, elected)])


def gain_stage(packets, where, leaves, low, high, earlier, plan):
    devices = packets.shape[0]
    picks = plan["picks"]
    units = high - low
    chunks = plan["chunks"]
    chunk = 4 if devices % 4 == 0 else 1
    even = plan["units"] % HALVES == 0

    half = cdiv(chunks, 2)
    batch = 4

    def body(where_ref, packet_ref, *refs):
        total_ref, grad_ref, hess_ref, late_ref = refs[-4:]
        out_ref = refs[len(before)]
        leaf_id = lax.broadcasted_iota(jnp.int32, (leaves, LANES), 0).astype(jnp.float32)
        bin_id = lax.broadcasted_iota(jnp.int32, (LANES, LANES), 0).astype(jnp.float32)
        local = []
        limit = []
        base = where_ref[0] % plan["owners"] * plan["units"]
        first = jnp.minimum(base // HALVES, plan["padded"] - picks)
        for i in range(low, high):
            if even:
                local.append(i // HALVES)
                limit.append(bin_id + float(i % HALVES * LANES))
            else:
                local.append(jnp.clip((base + i) // HALVES - first, 0, picks - 1))
                limit.append(bin_id + ((base + i) % HALVES * LANES).astype(jnp.float32))

        def terms(tiles):
            weights = []
            steps = [[] for _ in range(units)]
            grad_sum = jnp.zeros((leaves, LANES), jnp.float32)
            hess_sum = jnp.zeros((leaves, LANES), jnp.float32)
            for s, c, valid in tiles:
                owner = packet_ref[s, c, picks : picks + 1, :]
                if valid is not None:
                    owner = jnp.where(valid, owner, -1.0)
                mine = owner == leaf_id
                grad = jnp.where(mine, packet_ref[s, c, picks + 1 : picks + 2, :], 0.0)
                hess = jnp.where(mine, packet_ref[s, c, picks + 2 : picks + 3, :], 0.0)
                grad_sum = grad_sum + grad
                hess_sum = hess_sum + hess
                grad_high = grad.astype(jnp.bfloat16)
                hess_high = hess.astype(jnp.bfloat16)
                grad_low = (grad - grad_high.astype(jnp.float32)).astype(jnp.bfloat16)
                hess_low = (hess - hess_high.astype(jnp.float32)).astype(jnp.bfloat16)
                weights.append(
                    jnp.concatenate([grad_high, hess_high, grad_low, hess_low], axis=0)
                )
                for i in range(units):
                    value = packet_ref[s, c, pl.ds(local[i], 1), :]
                    steps[i].append((value <= limit[i]).astype(jnp.float32).astype(jnp.bfloat16))
            weight = jnp.concatenate(weights, axis=1)
            step = jnp.concatenate([jnp.concatenate(p, axis=1) for p in steps], axis=0)
            product = lax.dot_general(
                weight, step, (((1,), (1,)), ((), ())), preferred_element_type=jnp.float32
            )
            return product, grad_sum, hess_sum

        late = jnp.int32(0)
        for c in range(half, chunks):
            for s0 in range(0, devices, 16):
                flag = jnp.zeros((1, LANES), jnp.float32)
                for s in range(s0, min(s0 + 16, devices)):
                    row = plan["vote_lines"]
                    count = packet_ref[s, chunks + row // plan["rows"], row % plan["rows"], :]
                    flag = flag + jnp.where(
                        count.reshape(1, LANES) > float(c * LANES), float(1 << (s - s0)), 0.0
                    )
                flag = jnp.max(flag).astype(jnp.int32)
                for s in range(s0, min(s0 + 16, devices)):
                    late_ref[late] = s * chunks + c
                    late = late + (jnp.right_shift(flag, s - s0) & 1)

        def listed(first):
            tiles = []
            for k in range(batch):
                valid = first + k < late
                tile = jnp.where(valid, late_ref[first + k], 0)
                tiles.append((tile // chunks, tile % chunks, valid))
            return tiles

        total = grad_all = hess_all = None
        for s0 in range(0, devices + 1, chunk):
            if s0 < devices:
                tiles = [(s, c, None) for s in range(s0, s0 + chunk) for c in range(half)]
            else:
                tiles = listed(0)
            more, grad_more, hess_more = terms(tiles)
            if s0:
                more = total + more
                grad_more = grad_all + grad_more
                hess_more = hess_all + hess_more
            total, grad_all, hess_all = more, grad_more, hess_more
        total_ref[...] = total
        grad_ref[...] = grad_all
        hess_ref[...] = hess_all

        def add(k, carry):
            more, grad_more, hess_more = terms(listed(k * batch))
            total_ref[...] += more
            grad_ref[...] += grad_more
            hess_ref[...] += hess_more
            return carry

        lax.fori_loop(1, jnp.maximum((late + batch - 1) // batch, 1), add, 0)
        total = total_ref[...]
        grad_all = grad_ref[...]
        hess_all = hess_ref[...]
        prefix_grad = total[0:leaves] + total[2 * leaves : 3 * leaves]
        prefix_hess = total[leaves : 2 * leaves] + total[3 * leaves :]
        whole_grad = jnp.sum(grad_all, axis=1, keepdims=True)
        whole_hess = jnp.sum(hess_all, axis=1, keepdims=True)
        rest_grad = whole_grad - prefix_grad
        rest_hess = whole_hess - prefix_hess
        gains = (
            prefix_grad * prefix_grad / (prefix_hess + ridge_weight)
            + rest_grad * rest_grad / (rest_hess + ridge_weight)
            - whole_grad * whole_grad / (whole_hess + ridge_weight)
        )
        for i in range(units):
            out_ref[i * leaves : (i + 1) * leaves, :] = gains[:, i * LANES : (i + 1) * LANES]
        if before:
            whole_ref = refs[len(before) + 1]
            whole_ref[0 : low * leaves, :] = refs[0][...]
            whole_ref[low * leaves :, :] = out_ref[...]

    before = [] if earlier is None else [in_vmem(earlier)]
    shapes = [vmem_array((units * leaves, LANES))]
    if before:
        shapes.append(vmem_array((high * leaves, LANES)))
    vmem = pl.BlockSpec(memory_space=pltpu.VMEM)
    return pl.pallas_call(
        body,
        in_specs=[pl.BlockSpec(memory_space=pltpu.SMEM), vmem] + [vmem] * len(before),
        out_specs=[vmem] * len(shapes),
        out_shape=shapes,
        scratch_shapes=[
            pltpu.VMEM((4 * leaves, units * LANES), jnp.float32),
            pltpu.VMEM((leaves, LANES), jnp.float32),
            pltpu.VMEM((leaves, LANES), jnp.float32),
            pltpu.SMEM((devices * chunks + batch,), jnp.int32),
        ],
        compiler_params=pltpu.CompilerParams(vmem_limit_bytes=48 << 20),
        name="gain_stage",
    )(where, in_vmem(packets), *before)


def vote_stage(packets, before, sources, last, features, leaves, kept, plan):
    rows = plan["rows"]
    lines = plan["vote_lines"]
    step = 128
    depth = round_up(features, step)
    inputs = [in_vmem(packets)] + ([] if before is None else [in_vmem(before)])

    def body(packet_ref, *refs):
        out_ref, count = refs[-2:] if last else (None, refs[-1])
        lane = lax.broadcasted_iota(jnp.int32, (1, LANES), 1)

        feature = lax.broadcasted_iota(jnp.int32, (step, LANES), 0).astype(jnp.float32)
        feature = feature.astype(jnp.bfloat16)
        one = jnp.ones((step, LANES), jnp.bfloat16)
        zero = jnp.zeros((step, LANES), jnp.bfloat16)

        def block(index, carry):
            start = pl.multiple_of(index * step, step)
            offset = jnp.float32(index * step)
            total = jnp.zeros((step, LANES), jnp.float32)
            if before is not None:
                total = refs[0][pl.ds(start, step), :]
            for s0 in range(0, len(sources), 16):
                found = jnp.zeros((step, LANES), jnp.bfloat16)
                for s in sources[s0 : s0 + 16]:
                    for line in range(lines):
                        row = line % rows
                        values = packet_ref[s, plan["chunks"] + line // rows, row : row + 1, :]
                        inside = kept * leaves - line * LANES
                        if inside < LANES:
                            values = jnp.where(lane < inside, values, -1.0)
                        values = jnp.clip(values - offset, -1.0, float(step))
                        values = jnp.broadcast_to(values, (16, LANES)).astype(jnp.bfloat16)
                        values = jnp.concatenate([values] * (step // 16), axis=0)
                        found = found + jnp.where(values == feature, one, zero)
                total = total + found.astype(jnp.float32)
            count[pl.ds(start, step), :] = total
            return carry

        lax.fori_loop(0, depth // step, block, 0)
        if last:
            turned = count[...].T
            summed = turned[0:leaves]
            for i in range(1, LANES // leaves):
                summed = summed + turned[i * leaves : (i + 1) * leaves]
            out_ref[...] = summed[:, 0:features].astype(jnp.int32)

    vmem = pl.BlockSpec(memory_space=pltpu.VMEM)
    if last:
        out_shape = jax.ShapeDtypeStruct((leaves, features), jnp.int32)
        scratch = [pltpu.VMEM((depth, LANES), jnp.float32)]
    else:
        out_shape = vmem_array((depth, LANES))
        scratch = []
    return pl.pallas_call(
        body,
        in_specs=[vmem] * len(inputs),
        out_specs=vmem,
        out_shape=out_shape,
        scratch_shapes=scratch,
        compiler_params=pltpu.CompilerParams(vmem_limit_bytes=48 << 20),
        cost_estimate=pl.CostEstimate(flops=20_000_000, bytes_accessed=400_000, transcendentals=0),
        name="vote_stage",
    )(*inputs)


def pack_stage(arrays):
    def body(*refs):
        start = 0
        for ref in refs[:-1]:
            refs[-1][start : start + ref.shape[0], :] = ref[...]
            start += ref.shape[0]

    vmem = pl.BlockSpec(memory_space=pltpu.VMEM)
    return pl.pallas_call(
        body,
        in_specs=[vmem] * len(arrays),
        out_specs=vmem,
        out_shape=vmem_array((sum(a.shape[0] for a in arrays), arrays[0].shape[1])),
        compiler_params=pltpu.CompilerParams(vmem_limit_bytes=48 << 20),
        name="pack_stage",
    )(*[in_vmem(a) for a in arrays])


def place_stage(blocks, pieces, where, leaves, picked, plan):
    units = plan["units"]
    owners = plan["owners"]
    step = 8 if leaves % 8 == 0 else leaves

    rows = step * picked
    groups = leaves // step

    def body(where_ref, *refs):
        out_ref, planes, done = refs[-3:]
        here = where_ref[0] % owners
        odd = here & 1
        owner = []
        for _, _, even_tag, odd_tag, _, _, other in pieces:
            if not plan["doubling"]:
                owner.append(even_tag)
            elif not other:
                owner.append(here ^ jnp.where(odd == 1, odd_tag, even_tag))
            else:
                owner.append(here ^ 1 ^ jnp.where(odd == 1, even_tag, odd_tag))
        copies = []
        for g in range(groups):
            for index, (number, base, _, _, low, high, _) in enumerate(pieces):
                for i in range(low, high):

                    def write(index=index, ref=refs[number], i=i, low=low, base=base):
                        if units % HALVES == 0:
                            half = i % HALVES
                            pick = owner[index] * (units // HALVES) + i // HALVES
                        else:
                            half = (owner[index] * units + i) % HALVES
                            pick = (owner[index] * units + i) // HALVES
                        start = base + (i - low) * leaves + g * step
                        planes[half, pl.ds(g * rows + pick, step, stride=picked), :] = ref[
                            start : start + step, :
                        ]

                    if owners * units == picked * HALVES:
                        write()
                    else:
                        pl.when(owner[index] * units + i < picked * HALVES)(write)
            for half in range(HALVES):
                copy = pltpu.make_async_copy(
                    planes.at[half, pl.ds(g * rows, rows), :],
                    out_ref.at[pl.ds(g * rows, rows), pl.ds(half * LANES, LANES)],
                    done.at[g * HALVES + half],
                )
                copy.start()
                copies.append(copy)
        for copy in copies:
            copy.wait()

    vmem = pl.BlockSpec(memory_space=pltpu.VMEM)
    return pl.pallas_call(
        body,
        in_specs=[pl.BlockSpec(memory_space=pltpu.SMEM)] + [vmem] * len(blocks),
        out_specs=pl.BlockSpec(memory_space=pltpu.HBM),
        out_shape=jax.ShapeDtypeStruct((leaves * picked, B), jnp.float32),
        scratch_shapes=[
            pltpu.VMEM((HALVES, leaves * picked, LANES), jnp.float32),
            pltpu.SemaphoreType.DMA((groups * HALVES,)),
        ],
        compiler_params=pltpu.CompilerParams(vmem_limit_bytes=48 << 20),
        name="place_stage",
    )(where, *[in_vmem(b) for b in blocks]).reshape(leaves, picked, B)


def solution(mesh):
    devices = mesh.shape["rows"]

    def on_device(
        feature_bin, doc_leaf, current_score, relevance, doc_rank, query_length, feature_votes,
        elected,
    ):
        documents, features = feature_bin.shape
        leaves, picked = elected.shape
        kept = feature_votes.shape[2]
        doubling = devices >= 8 and devices & (devices - 1) == 0
        owners = devices // 2 if doubling else devices
        units = max(cdiv(picked * HALVES, owners), 2)
        padded = round_up(picked, 8)
        picks = max(
            (j * units + units - 1) // HALVES - (j * units) // HALVES + 1 for j in range(owners)
        )
        rows = round_up(picks + 3, 8)
        plan = {
            "devices": devices,
            "doubling": doubling,
            "owners": owners,
            "units": units,
            "picks": picks,
            "padded": padded,
            "first": [min(j * units // HALVES, padded - picks) for j in range(owners)],
            "rows": rows,
            "chunks": documents // LANES,
            "vote_lines": cdiv(kept * leaves, LANES),
            "vote_tiles": cdiv(cdiv(kept * leaves, LANES) + 1, rows),
        }
        where = lax.axis_index("rows").astype(jnp.int32).reshape(1)
        gradient, hessian, packets = local_stage(
            feature_bin.T,
            doc_leaf.reshape(1, -1),
            current_score.reshape(1, -1),
            relevance.reshape(1, -1),
            doc_rank.reshape(1, -1),
            query_length,
            feature_votes.transpose(2, 0, 1),
            elected,
            plan,
        )
        received = lax.all_to_all(packets, "rows", 0, 0)
        counters = (features, leaves, kept, plan)
        third = cdiv(devices, 3)
        shares = [range(min(k * third, devices), min((k + 1) * third, devices)) for k in range(3)]
        cut = units * 4 // 5
        if units % HALVES == 0:
            cut = max(cut // HALVES, 1) * HALVES if units > HALVES else 1
        (part,) = gain_stage(received, where, leaves, 0, cut, None, plan)
        rest, block = gain_stage(received, where, leaves, cut, units, part, plan)
        votes = vote_stage(received, None, shares[0], False, *counters)
        if doubling:
            far = [1 << b for b in reversed(range(1, owners.bit_length() - 1))]
            twin = list(far)
            twin[-2:] = twin[-2:][::-1]
            pairs = [
                [(i, i ^ (twin[p] if i & 1 else far[p])) for i in range(devices)]
                for p in range(len(far))
            ]
            sibling = [(i, i ^ 1) for i in range(devices)]

            def send(items, p):
                return [
                    (
                        lax.ppermute(b, "rows", pairs[p]),
                        [(even ^ far[p], odd ^ twin[p], low, high) for even, odd, low, high in spans],
                    )
                    for b, spans in items
                ]

            def cross(items):
                return [(lax.ppermute(b, "rows", sibling), spans) for b, spans in items]

            def after(items, other):
                arrays, other = lax.optimization_barrier(([item[0] for item in items], other))
                return [(b, item[1]) for b, item in zip(arrays, items)], other

            def packed_after(items, votes):
                packed = pack_stage([b for b, _ in items])
                packed = (packed, sum([spans for _, spans in items], []))
                return after([packed], votes)

            own = [(block, [(0, 0, 0, units)])]
            first = send([(part, [(0, 0, 0, cut)])], 0)
            second = send([(rest, [(0, 0, cut, units)])], 0)
            first, votes = after(first, votes)
            votes = vote_stage(received, votes, shares[1], False, *counters)
            items = own + first + second
            for p in range(1, len(far)):
                if p < len(far) - 1:
                    items = items + send(items, p)
                    continue
                moved = send(own, p)
                moved = moved + send(items[1:-1], p)
                moved = moved + send(items[-1:], p)
                votes = vote_stage(received, votes, shares[2], True, *counters)
                packed, votes = packed_after(items, votes)
                crossed = cross(packed)
                crossed = crossed + cross(moved[:1])
                crossed = crossed + cross(moved[1:-1])
                crossed = crossed + cross(moved[-1:])
                items = items + moved
            if len(far) == 1:
                votes = vote_stage(received, votes, shares[2], True, *counters)
                crossed = cross(items)
            pieces = []
            blocks = []
            for side, group in ((False, items), (True, crossed)):
                for b, spans in group:
                    base = 0
                    for even, odd, low, high in spans:
                        pieces.append((len(blocks), base, even, odd, low, high, side))
                        base += (high - low) * leaves
                    blocks.append(b)
        else:
            votes = vote_stage(received, votes, range(third, devices), True, *counters)
            gathered = lax.all_gather(block, "rows", axis=0)
            blocks = [gathered[j] for j in range(devices)]
            pieces = [(j, 0, j, j, 0, units, False) for j in range(devices)]
        split_gain = place_stage(blocks, pieces, where, leaves, picked, plan)
        return gradient.reshape(-1), hessian.reshape(-1), votes, split_gain


    return jax.shard_map(
        on_device,
        mesh=mesh,
        in_specs=(
            P(("parts", "rows"), None),
            P(("parts", "rows")),
            P(("parts", "rows")),
            P(("parts", "rows")),
            P(("parts", "rows")),
            P(("parts", "rows")),
            P(("parts", "rows"), None, None),
            P("parts", None),
        ),
        out_specs=(
            P(("parts", "rows")),
            P(("parts", "rows")),
            P("parts", None),
            P("parts", None, None),
        ),
        check_vma=False,
    )
```

```python
import jax
import jax.numpy as jnp
from jax import lax
from jax.experimental import pallas as pl
from jax.experimental.pallas import tpu as pltpu
from jax.sharding import PartitionSpec as P


B = 256
LANES = 128
HALVES = B // LANES
LEVELS = 4

ridge_weight = 1.0


def cdiv(a, b):
    return -(-a // b)


def round_up(a, b):
    return cdiv(a, b) * b


def query_rows(score, level, rank, lengths, slots):
    documents = score.shape[1]
    queries = documents // slots
    gain = jnp.left_shift(1, level).astype(jnp.float32) - 1.0
    discount = 1.0 / jnp.log2(rank.astype(jnp.float32) + 2.0)
    place = lax.broadcasted_iota(jnp.int32, (1, slots), 1)
    place_discount = 1.0 / jnp.log2(place.astype(jnp.float32) + 2.0)
    gradients = []
    hessians = []
    for q in range(queries):
        lanes = slice(q * slots, (q + 1) * slots)
        live = place < lengths[q]
        live_row = live.astype(jnp.float32)
        score_row = score[:, lanes]
        gain_row = gain[:, lanes]
        discount_row = discount[:, lanes]
        level_row = jnp.where(live, level[:, lanes], -1)
        ideal_gain = jnp.zeros((1, slots), jnp.float32)
        for v in range(1, LEVELS + 1):
            count = jnp.sum((level_row >= v).astype(jnp.float32), axis=1, keepdims=True)
            ideal_gain = ideal_gain + jnp.where(
                place.astype(jnp.float32) < count, float(2 ** (v - 1)), 0.0
            )
        ideal = jnp.sum(ideal_gain * place_discount, axis=1, keepdims=True)
        scaling = 1.0 / jnp.maximum(ideal, 1.0)
        rows = jnp.concatenate(
            [score_row, gain_row, discount_row, live_row, jnp.zeros((4, slots), jnp.float32)],
            axis=0,
        )
        columns = rows.T
        step = 32
        push_sum = jnp.zeros((8, slots), jnp.float32)
        curve_sum = jnp.zeros((8, slots), jnp.float32)
        for r in range(0, slots, step):
            part = columns[r : r + step]
            gap = (part[:, 1:2] - gain_row) * part[:, 3:4]
            change = gap * jnp.abs(part[:, 2:3] - discount_row)
            lead = score_row - part[:, 0:1]
            chance = 1.0 / (1.0 + jnp.exp(jnp.where(gap > 0.0, -lead, lead)))
            push = chance * change
            curve = (1.0 - chance) * jnp.abs(push)
            for k in range(0, step, 8):
                push_sum = push_sum + push[k : k + 8]
                curve_sum = curve_sum + curve[k : k + 8]
        factor = scaling * live_row
        gradients.append(jnp.sum(push_sum, axis=0, keepdims=True) * factor)
        hessians.append(jnp.sum(curve_sum, axis=0, keepdims=True) * factor)
    return jnp.concatenate(gradients, axis=1), jnp.concatenate(hessians, axis=1)


def vmem_array(shape):
    return pltpu.VMEM(shape, jnp.float32)


def in_vmem(x):
    return pltpu.with_memory_space_constraint(x, pltpu.VMEM)


def in_hbm(x):
    return pltpu.with_memory_space_constraint(x, pltpu.HBM)


def local_stage(bins, leaf, score, level, rank, lengths, votes, elected, plan):
    features, documents = bins.shape
    leaves, picked = elected.shape
    kept = votes.shape[0]
    padded = plan["padded"]
    picks = plan["picks"]
    rows = plan["rows"]
    slots = documents // lengths.shape[0]
    group = 8 if leaves % 8 == 0 else leaves
    per_row = LANES // leaves

    piece = round_up(cdiv(features, 4), 8)
    cuts = [(f, min(piece, features - f)) for f in range(0, features, piece)]

    def body(*refs):
        sources = refs[0:8]
        grad_ref, hess_ref, packet_ref = refs[8:11]
        square, chosen_ref = refs[11:13]
        copied = refs[13:21]
        arrived = refs[21]
        bins_here, leaf_ref, score_ref, level_ref, rank_ref, length_ref, votes_ref, elected_ref = (
            copied
        )
        small = [
            pltpu.make_async_copy(sources[k], copied[k], arrived.at[len(cuts) + k - 1])
            for k in (5, 2, 3, 4, 7, 1, 6)
        ]
        fetches = [
            pltpu.make_async_copy(
                sources[0].at[pl.ds(f, size), :], bins_here.at[pl.ds(f, size), :], arrived.at[k]
            )
            for k, (f, size) in enumerate(cuts)
        ]
        for copy in small + fetches:
            copy.start()
        for copy in small:
            copy.wait()
        square[...] = jnp.zeros(square.shape, jnp.float32)
        square[0:leaves, 0:picked] = elected_ref[...].astype(jnp.float32)
        elected_t = square[...].T
        leaf_row = leaf_ref[...]
        gradient, hessian = query_rows(
            score_ref[...], level_ref[...], rank_ref[...], length_ref, slots
        )
        grad_ref[...] = gradient
        hess_ref[...] = hessian
        lane = lax.broadcasted_iota(jnp.int32, (1, documents), 1)
        starts = [0]
        for q in range(documents // slots):
            starts.append(starts[-1] + length_ref[q])

        def compact(block):
            result = block
            for q in range(1, documents // slots):
                moved = pltpu.roll(block, starts[q] - q * slots + documents, 1)
                result = jnp.where(lane >= starts[q], moved, result)
            return result

        shared = [leaf_row.astype(jnp.float32), gradient, hessian]
        shared.append(jnp.zeros((max(rows - picks, 8) - 3, documents), jnp.float32))
        shared = compact(jnp.concatenate(shared, axis=0))[0 : rows - picks]
        shared = jnp.where(lane < starts[-1], shared, 0.0)
        count = jnp.zeros((1, LANES), jnp.float32) + starts[-1].astype(jnp.float32)
        feature = lax.broadcasted_iota(jnp.int32, (padded, features), 1).astype(jnp.float32)
        for fetch in fetches:
            fetch.wait()
        table = bins_here[...].astype(jnp.float32).astype(jnp.bfloat16)
        chosen = jnp.zeros((padded, documents), jnp.float32)
        for first in range(0, leaves, group):
            hot = []
            for l in range(first, first + group):
                hot.append((elected_t[0:padded, l : l + 1] == feature).astype(jnp.float32))
            hot = jnp.concatenate(hot, axis=0).astype(jnp.bfloat16)
            found = jnp.dot(hot, table, preferred_element_type=jnp.float32)
            for i in range(group):
                chosen = jnp.where(
                    leaf_row == first + i, found[i * padded : (i + 1) * padded], chosen
                )
        chosen_ref[...] = compact(chosen)
        tail = []
        for k0 in range(0, kept, per_row):
            line = jnp.zeros((1, LANES), jnp.float32)
            for i in range(min(per_row, kept - k0)):
                values = votes_ref[k0 + i].astype(jnp.float32)
                pieces = [values]
                if i:
                    pieces.insert(0, jnp.zeros((1, i * leaves), jnp.float32))
                if (i + 1) * leaves < LANES:
                    pieces.append(jnp.zeros((1, LANES - (i + 1) * leaves), jnp.float32))
                line = line + jnp.concatenate(pieces, axis=1)
            tail.append(line)
        tail.append(count)
        spare = plan["vote_tiles"] * rows - len(tail)
        if spare:
            tail.append(jnp.zeros((spare, LANES), jnp.float32))
        tail = jnp.concatenate(tail, axis=0)
        for j in range(plan["devices"]):
            start = plan["first"][j % plan["owners"]]
            block = jnp.concatenate([chosen_ref[start : start + picks, :], shared], axis=0)
            for c in range(documents // LANES):
                packet_ref[j, c] = block[:, c * LANES : (c + 1) * LANES]
            for t in range(plan["vote_tiles"]):
                packet_ref[j, documents // LANES + t] = tail[t * rows : (t + 1) * rows]

    vmem = pl.BlockSpec(memory_space=pltpu.VMEM)
    return pl.pallas_call(
        body,
        in_specs=[pl.BlockSpec(memory_space=pltpu.HBM)] * 8,
        out_specs=[vmem] * 3,
        out_shape=[
            jax.ShapeDtypeStruct((1, documents), jnp.float32),
            jax.ShapeDtypeStruct((1, documents), jnp.float32),
            vmem_array(
                (plan["devices"], documents // LANES + plan["vote_tiles"], rows, LANES)
            ),
        ],
        scratch_shapes=[
            pltpu.VMEM((LANES, LANES), jnp.float32),
            pltpu.VMEM((padded, documents), jnp.float32),
            pltpu.VMEM((features, documents), jnp.int32),
            pltpu.VMEM((1, documents), jnp.int32),
            pltpu.VMEM((1, documents), jnp.float32),
            pltpu.VMEM((1, documents), jnp.int32),
            pltpu.VMEM((1, documents), jnp.int32),
            pltpu.SMEM(lengths.shape, jnp.int32),
            pltpu.VMEM(votes.shape, jnp.int32),
            pltpu.VMEM(elected.shape, jnp.int32),
            pltpu.SemaphoreType.DMA((len(cuts) + 7,)),
        ],
        compiler_params=pltpu.CompilerParams(vmem_limit_bytes=48 << 20),
        name="local_stage",
    )(*[in_hbm(x) for x in (bins, leaf, score, level, rank, lengths, votes, elected)])


def gain_stage(packets, where, leaves, low, high, earlier, plan):
    devices = packets.shape[0]
    picks = plan["picks"]
    units = high - low
    chunks = plan["chunks"]
    chunk = 4 if devices % 4 == 0 else 1
    even = plan["units"] % HALVES == 0
    plain = units // 2 // HALVES * HALVES if even else 0

    half = cdiv(chunks, 2)
    batch = 4

    def body(where_ref, packet_ref, *refs):
        total_ref, grad_ref, hess_ref, late_ref = refs[-4:]
        out_ref = refs[len(before)]
        leaf_id = lax.broadcasted_iota(jnp.int32, (leaves, LANES), 0).astype(jnp.float32)
        bin_id = lax.broadcasted_iota(jnp.int32, (LANES, LANES), 0).astype(jnp.float32)
        across = lax.broadcasted_iota(jnp.int32, (LANES, LANES), 1).astype(jnp.float32)
        local = []
        limit = []
        base = where_ref[0] % plan["owners"] * plan["units"]
        first = jnp.minimum(base // HALVES, plan["padded"] - picks)
        for i in range(low, high):
            if even:
                local.append(i // HALVES)
                limit.append((across if i - low < plain else bin_id) + float(i % HALVES * LANES))
            else:
                local.append(jnp.clip((base + i) // HALVES - first, 0, picks - 1))
                limit.append(bin_id + ((base + i) % HALVES * LANES).astype(jnp.float32))

        def turned(tiles):
            rows = plan["rows"]
            result = []
            for t0 in range(0, len(tiles), LANES // rows):
                some = [packet_ref[s, c] for s, c, _ in tiles[t0 : t0 + LANES // rows]]
                spare = LANES - len(some) * rows
                if spare:
                    some.append(jnp.zeros((spare, LANES), jnp.float32))
                square = jnp.concatenate(some, axis=0).T
                for t in range(min(len(tiles) - t0, LANES // rows)):
                    result.append(square[:, t * rows : (t + 1) * rows])
            return result

        def terms(tiles):
            weights = []
            steps = []
            others = [[] for _ in range(units - plain)]
            columns = turned(tiles) if plain else [None] * len(tiles)
            grad_sum = jnp.zeros((leaves, LANES), jnp.float32)
            hess_sum = jnp.zeros((leaves, LANES), jnp.float32)
            for (s, c, valid), column in zip(tiles, columns):
                owner = packet_ref[s, c, picks : picks + 1, :]
                if valid is not None:
                    owner = jnp.where(valid, owner, -1.0)
                mine = owner == leaf_id
                grad = jnp.where(mine, packet_ref[s, c, picks + 1 : picks + 2, :], 0.0)
                hess = jnp.where(mine, packet_ref[s, c, picks + 2 : picks + 3, :], 0.0)
                grad_sum = grad_sum + grad
                hess_sum = hess_sum + hess
                grad_high = grad.astype(jnp.bfloat16)
                hess_high = hess.astype(jnp.bfloat16)
                grad_low = (grad - grad_high.astype(jnp.float32)).astype(jnp.bfloat16)
                hess_low = (hess - hess_high.astype(jnp.float32)).astype(jnp.bfloat16)
                weights.append(
                    jnp.concatenate([grad_high, hess_high, grad_low, hess_low], axis=0)
                )
                step = []
                for i in range(plain):
                    k = local[i]
                    value = jnp.broadcast_to(column[:, k : k + 1], (LANES, LANES))
                    step.append((value <= limit[i]).astype(jnp.float32).astype(jnp.bfloat16))
                if plain:
                    steps.append(jnp.concatenate(step, axis=1))
                for i in range(plain, units):
                    value = packet_ref[s, c, pl.ds(local[i], 1), :]
                    others[i - plain].append(
                        (value <= limit[i]).astype(jnp.float32).astype(jnp.bfloat16)
                    )
            weight = jnp.concatenate(weights, axis=1)
            product = []
            if plain:
                step = jnp.concatenate(steps, axis=0)
                product.append(jnp.dot(weight, step, preferred_element_type=jnp.float32))
            if plain < units:
                step = jnp.concatenate([jnp.concatenate(p, axis=1) for p in others], axis=0)
                product.append(
                    lax.dot_general(
                        weight,
                        step,
                        (((1,), (1,)), ((), ())),
                        preferred_element_type=jnp.float32,
                    )
                )
            product = jnp.concatenate(product, axis=1)
            return product, grad_sum, hess_sum

        late = jnp.int32(0)
        for c in range(half, chunks):
            for s0 in range(0, devices, 16):
                flag = jnp.zeros((1, LANES), jnp.float32)
                for s in range(s0, min(s0 + 16, devices)):
                    row = plan["vote_lines"]
                    count = packet_ref[s, chunks + row // plan["rows"], row % plan["rows"], :]
                    flag = flag + jnp.where(
                        count.reshape(1, LANES) > float(c * LANES), float(1 << (s - s0)), 0.0
                    )
                flag = jnp.max(flag).astype(jnp.int32)
                for s in range(s0, min(s0 + 16, devices)):
                    late_ref[late] = s * chunks + c
                    late = late + (jnp.right_shift(flag, s - s0) & 1)

        def listed(first):
            tiles = []
            for k in range(batch):
                valid = first + k < late
                tile = jnp.where(valid, late_ref[first + k], 0)
                tiles.append((tile // chunks, tile % chunks, valid))
            return tiles

        total = grad_all = hess_all = None
        for s0 in range(0, devices + 1, chunk):
            if s0 < devices:
                tiles = [(s, c, None) for s in range(s0, s0 + chunk) for c in range(half)]
            else:
                tiles = listed(0)
            more, grad_more, hess_more = terms(tiles)
            if s0:
                more = total + more
                grad_more = grad_all + grad_more
                hess_more = hess_all + hess_more
            total, grad_all, hess_all = more, grad_more, hess_more
        total_ref[...] = total
        grad_ref[...] = grad_all
        hess_ref[...] = hess_all

        def add(k, carry):
            more, grad_more, hess_more = terms(listed(k * batch))
            total_ref[...] += more
            grad_ref[...] += grad_more
            hess_ref[...] += hess_more
            return carry

        lax.fori_loop(1, jnp.maximum((late + batch - 1) // batch, 1), add, 0)
        total = total_ref[...]
        grad_all = grad_ref[...]
        hess_all = hess_ref[...]
        prefix_grad = total[0:leaves] + total[2 * leaves : 3 * leaves]
        prefix_hess = total[leaves : 2 * leaves] + total[3 * leaves :]
        whole_grad = jnp.sum(grad_all, axis=1, keepdims=True)
        whole_hess = jnp.sum(hess_all, axis=1, keepdims=True)
        rest_grad = whole_grad - prefix_grad
        rest_hess = whole_hess - prefix_hess
        gains = (
            prefix_grad * prefix_grad / (prefix_hess + ridge_weight)
            + rest_grad * rest_grad / (rest_hess + ridge_weight)
            - whole_grad * whole_grad / (whole_hess + ridge_weight)
        )
        for i in range(units):
            out_ref[i * leaves : (i + 1) * leaves, :] = gains[:, i * LANES : (i + 1) * LANES]
        if before:
            whole_ref = refs[len(before) + 1]
            whole_ref[0 : low * leaves, :] = refs[0][...]
            whole_ref[low * leaves :, :] = out_ref[...]

    before = [] if earlier is None else [in_vmem(earlier)]
    shapes = [vmem_array((units * leaves, LANES))]
    if before:
        shapes.append(vmem_array((high * leaves, LANES)))
    vmem = pl.BlockSpec(memory_space=pltpu.VMEM)
    return pl.pallas_call(
        body,
        in_specs=[pl.BlockSpec(memory_space=pltpu.SMEM), vmem] + [vmem] * len(before),
        out_specs=[vmem] * len(shapes),
        out_shape=shapes,
        scratch_shapes=[
            pltpu.VMEM((4 * leaves, units * LANES), jnp.float32),
            pltpu.VMEM((leaves, LANES), jnp.float32),
            pltpu.VMEM((leaves, LANES), jnp.float32),
            pltpu.SMEM((devices * chunks + batch,), jnp.int32),
        ],
        compiler_params=pltpu.CompilerParams(vmem_limit_bytes=48 << 20),
        name="gain_stage",
    )(where, in_vmem(packets), *before)


def vote_stage(packets, before, sources, last, features, leaves, kept, plan):
    rows = plan["rows"]
    lines = plan["vote_lines"]
    step = 128
    depth = round_up(features, step)
    inputs = [in_vmem(packets)] + ([] if before is None else [in_vmem(before)])

    def body(packet_ref, *refs):
        out_ref, count = refs[-2:] if last else (None, refs[-1])
        lane = lax.broadcasted_iota(jnp.int32, (1, LANES), 1)

        feature = lax.broadcasted_iota(jnp.int32, (step, LANES), 0).astype(jnp.float32)
        feature = feature.astype(jnp.bfloat16)
        one = jnp.ones((step, LANES), jnp.bfloat16)
        zero = jnp.zeros((step, LANES), jnp.bfloat16)

        def block(index, carry):
            start = pl.multiple_of(index * step, step)
            offset = jnp.float32(index * step)
            total = jnp.zeros((step, LANES), jnp.float32)
            if before is not None:
                total = refs[0][pl.ds(start, step), :]
            for s0 in range(0, len(sources), 16):
                found = jnp.zeros((step, LANES), jnp.bfloat16)
                for s in sources[s0 : s0 + 16]:
                    for line in range(lines):
                        row = line % rows
                        values = packet_ref[s, plan["chunks"] + line // rows, row : row + 1, :]
                        inside = kept * leaves - line * LANES
                        if inside < LANES:
                            values = jnp.where(lane < inside, values, -1.0)
                        values = jnp.clip(values - offset, -1.0, float(step))
                        values = jnp.broadcast_to(values, (16, LANES)).astype(jnp.bfloat16)
                        values = jnp.concatenate([values] * (step // 16), axis=0)
                        found = found + jnp.where(values == feature, one, zero)
                total = total + found.astype(jnp.float32)
            count[pl.ds(start, step), :] = total
            return carry

        lax.fori_loop(0, depth // step, block, 0)
        if last:
            turned = count[...].T
            summed = turned[0:leaves]
            for i in range(1, LANES // leaves):
                summed = summed + turned[i * leaves : (i + 1) * leaves]
            out_ref[...] = summed[:, 0:features].astype(jnp.int32)

    vmem = pl.BlockSpec(memory_space=pltpu.VMEM)
    if last:
        out_shape = jax.ShapeDtypeStruct((leaves, features), jnp.int32)
        scratch = [pltpu.VMEM((depth, LANES), jnp.float32)]
    else:
        out_shape = vmem_array((depth, LANES))
        scratch = []
    return pl.pallas_call(
        body,
        in_specs=[vmem] * len(inputs),
        out_specs=vmem,
        out_shape=out_shape,
        scratch_shapes=scratch,
        compiler_params=pltpu.CompilerParams(vmem_limit_bytes=48 << 20),
        cost_estimate=pl.CostEstimate(flops=20_000_000, bytes_accessed=400_000, transcendentals=0),
        name="vote_stage",
    )(*inputs)


def pack_stage(arrays):
    def body(*refs):
        start = 0
        for ref in refs[:-1]:
            refs[-1][start : start + ref.shape[0], :] = ref[...]
            start += ref.shape[0]

    vmem = pl.BlockSpec(memory_space=pltpu.VMEM)
    return pl.pallas_call(
        body,
        in_specs=[vmem] * len(arrays),
        out_specs=vmem,
        out_shape=vmem_array((sum(a.shape[0] for a in arrays), arrays[0].shape[1])),
        compiler_params=pltpu.CompilerParams(vmem_limit_bytes=48 << 20),
        name="pack_stage",
    )(*[in_vmem(a) for a in arrays])


def place_stage(blocks, pieces, where, leaves, picked, plan):
    units = plan["units"]
    owners = plan["owners"]
    step = 8 if leaves % 8 == 0 else leaves

    rows = step * picked
    groups = leaves // step

    def body(where_ref, *refs):
        out_ref, planes, done = refs[-3:]
        here = where_ref[0] % owners
        odd = here & 1
        owner = []
        for _, _, even_tag, odd_tag, _, _, other in pieces:
            if not plan["doubling"]:
                owner.append(even_tag)
            elif not other:
                owner.append(here ^ jnp.where(odd == 1, odd_tag, even_tag))
            else:
                owner.append(here ^ 1 ^ jnp.where(odd == 1, even_tag, odd_tag))
        copies = []
        for g in range(groups):
            for index, (number, base, _, _, low, high, _) in enumerate(pieces):
                for i in range(low, high):

                    def write(index=index, ref=refs[number], i=i, low=low, base=base):
                        if units % HALVES == 0:
                            half = i % HALVES
                            pick = owner[index] * (units // HALVES) + i // HALVES
                        else:
                            half = (owner[index] * units + i) % HALVES
                            pick = (owner[index] * units + i) // HALVES
                        start = base + (i - low) * leaves + g * step
                        planes[half, pl.ds(g * rows + pick, step, stride=picked), :] = ref[
                            start : start + step, :
                        ]

                    if owners * units == picked * HALVES:
                        write()
                    else:
                        pl.when(owner[index] * units + i < picked * HALVES)(write)
            for half in range(HALVES):
                copy = pltpu.make_async_copy(
                    planes.at[half, pl.ds(g * rows, rows), :],
                    out_ref.at[pl.ds(g * rows, rows), pl.ds(half * LANES, LANES)],
                    done.at[g * HALVES + half],
                )
                copy.start()
                copies.append(copy)
        for copy in copies:
            copy.wait()

    vmem = pl.BlockSpec(memory_space=pltpu.VMEM)
    return pl.pallas_call(
        body,
        in_specs=[pl.BlockSpec(memory_space=pltpu.SMEM)] + [vmem] * len(blocks),
        out_specs=pl.BlockSpec(memory_space=pltpu.HBM),
        out_shape=jax.ShapeDtypeStruct((leaves * picked, B), jnp.float32),
        scratch_shapes=[
            pltpu.VMEM((HALVES, leaves * picked, LANES), jnp.float32),
            pltpu.SemaphoreType.DMA((groups * HALVES,)),
        ],
        compiler_params=pltpu.CompilerParams(vmem_limit_bytes=48 << 20),
        name="place_stage",
    )(where, *[in_vmem(b) for b in blocks]).reshape(leaves, picked, B)


def solution(mesh):
    devices = mesh.shape["rows"]

    def on_device(
        feature_bin, doc_leaf, current_score, relevance, doc_rank, query_length, feature_votes,
        elected,
    ):
        documents, features = feature_bin.shape
        leaves, picked = elected.shape
        kept = feature_votes.shape[2]
        doubling = devices >= 8 and devices & (devices - 1) == 0
        owners = devices // 2 if doubling else devices
        units = max(cdiv(picked * HALVES, owners), 2)
        padded = round_up(picked, 8)
        picks = max(
            (j * units + units - 1) // HALVES - (j * units) // HALVES + 1 for j in range(owners)
        )
        rows = round_up(picks + 3, 8)
        plan = {
            "devices": devices,
            "doubling": doubling,
            "owners": owners,
            "units": units,
            "picks": picks,
            "padded": padded,
            "first": [min(j * units // HALVES, padded - picks) for j in range(owners)],
            "rows": rows,
            "chunks": documents // LANES,
            "vote_lines": cdiv(kept * leaves, LANES),
            "vote_tiles": cdiv(cdiv(kept * leaves, LANES) + 1, rows),
        }
        where = lax.axis_index("rows").astype(jnp.int32).reshape(1)
        gradient, hessian, packets = local_stage(
            feature_bin.T,
            doc_leaf.reshape(1, -1),
            current_score.reshape(1, -1),
            relevance.reshape(1, -1),
            doc_rank.reshape(1, -1),
            query_length,
            feature_votes.transpose(2, 0, 1),
            elected,
            plan,
        )
        received = lax.all_to_all(packets, "rows", 0, 0)
        counters = (features, leaves, kept, plan)
        third = cdiv(devices, 3)
        shares = [range(min(k * third, devices), min((k + 1) * third, devices)) for k in range(3)]
        cut = units * 4 // 5
        if units % HALVES == 0:
            cut = max(cut // HALVES, 1) * HALVES if units > HALVES else 1
        (part,) = gain_stage(received, where, leaves, 0, cut, None, plan)
        rest, block = gain_stage(received, where, leaves, cut, units, part, plan)
        votes = vote_stage(received, None, shares[0], False, *counters)
        if doubling:
            far = [1 << b for b in reversed(range(1, owners.bit_length() - 1))]
            twin = list(far)
            twin[-2:] = twin[-2:][::-1]
            pairs = [
                [(i, i ^ (twin[p] if i & 1 else far[p])) for i in range(devices)]
                for p in range(len(far))
            ]
            sibling = [(i, i ^ 1) for i in range(devices)]

            def send(items, p):
                return [
                    (
                        lax.ppermute(b, "rows", pairs[p]),
                        [(even ^ far[p], odd ^ twin[p], low, high) for even, odd, low, high in spans],
                    )
                    for b, spans in items
                ]

            def cross(items):
                return [(lax.ppermute(b, "rows", sibling), spans) for b, spans in items]

            def after(items, other):
                arrays, other = lax.optimization_barrier(([item[0] for item in items], other))
                return [(b, item[1]) for b, item in zip(arrays, items)], other

            def packed_after(items, votes):
                packed = pack_stage([b for b, _ in items])
                packed = (packed, sum([spans for _, spans in items], []))
                return after([packed], votes)

            own = [(block, [(0, 0, 0, units)])]
            first = send([(part, [(0, 0, 0, cut)])], 0)
            second = send([(rest, [(0, 0, cut, units)])], 0)
            first, votes = after(first, votes)
            votes = vote_stage(received, votes, shares[1], False, *counters)
            items = own + first + second
            for p in range(1, len(far)):
                if p < len(far) - 1:
                    items = items + send(items, p)
                    continue
                moved = send(own, p)
                moved = moved + send(items[1:-1], p)
                moved = moved + send(items[-1:], p)
                votes = vote_stage(received, votes, shares[2], True, *counters)
                packed, votes = packed_after(items, votes)
                crossed = cross(packed)
                crossed = crossed + cross(moved[:1])
                crossed = crossed + cross(moved[1:-1])
                crossed = crossed + cross(moved[-1:])
                items = items + moved
            if len(far) == 1:
                votes = vote_stage(received, votes, shares[2], True, *counters)
                crossed = cross(items)
            pieces = []
            blocks = []
            for side, group in ((False, items), (True, crossed)):
                for b, spans in group:
                    base = 0
                    for even, odd, low, high in spans:
                        pieces.append((len(blocks), base, even, odd, low, high, side))
                        base += (high - low) * leaves
                    blocks.append(b)
        else:
            votes = vote_stage(received, votes, range(third, devices), True, *counters)
            gathered = lax.all_gather(block, "rows", axis=0)
            blocks = [gathered[j] for j in range(devices)]
            pieces = [(j, 0, j, j, 0, units, False) for j in range(devices)]
        split_gain = place_stage(blocks, pieces, where, leaves, picked, plan)
        return gradient.reshape(-1), hessian.reshape(-1), votes, split_gain


    return jax.shard_map(
        on_device,
        mesh=mesh,
        in_specs=(
            P(("parts", "rows"), None),
            P(("parts", "rows")),
            P(("parts", "rows")),
            P(("parts", "rows")),
            P(("parts", "rows")),
            P(("parts", "rows")),
            P(("parts", "rows"), None, None),
            P("parts", None),
        ),
        out_specs=(
            P(("parts", "rows")),
            P(("parts", "rows")),
            P("parts", None),
            P("parts", None, None),
        ),
        check_vma=False,
    )
```
